8 devices in a mesh: tp: 1 (over z), cp: 8 (over y, x, core).
Axes of the slice: x: 2, y: 2, z: 1, core: 2. Of those that a mesh axis runs over, the one named last changes fastest.
Arguments:
- query: bfloat16 [32, 256, 4, 128], P(None, 'cp', 'tp')
- out_act: bfloat16 [32, 256, 4, 128], P(None, 'cp', 'tp')
- out_grad: bfloat16 [32, 256, 4, 128], P(None, 'cp', 'tp')
- row_lse: float32 [32, 256, 4], P(None, 'cp', 'tp')
- key_act: bfloat16 [8704, 1, 128], P('cp', 'tp')
- value_act: bfloat16 [8704, 1, 128], P('cp', 'tp')
- doc_ids: int32 [8704], replicated
Outputs:
- output 1: bfloat16 [32, 256, 4, 128], P(None, 'cp', 'tp')
- output 2: float32 [8704, 1, 128], P('cp', 'tp')
- output 3: float32 [8704, 1, 128], P('cp', 'tp')
All inputs are finite; a program needn't handle non-finite values.
Results may differ from the reference program's by a relative error of at most 0.001.
Values are sent between devices in bfloat16 or wider.
A program may use at most 1 GiB of HBM per device.

```python
import jax
import jax.numpy as jnp
from jax import lax

SLICES = 32
SUB_LEN = 256
PRE_LEN = 512
Q_HEADS = 4
KV_HEADS = 1
HEAD_DIM = 128
SPLITS = 8

PREFIX = PRE_LEN + SLICES * SUB_LEN
GROUP_SIZE = Q_HEADS // KV_HEADS
BLOCK_LEN = SUB_LEN // SPLITS
SCORE_SCALE = HEAD_DIM ** -0.5
GRAD_SCALE = (PREFIX // 8) ** 0.5
DOC_MEAN = PREFIX // 8


def masked_scores(q_blk, key_act, doc_ids, first_pos):
    block_len = q_blk.shape[0]
    scores = jnp.einsum('qhgd,khd->qhgk', q_blk.astype(jnp.float32), key_act.astype(jnp.float32)) * SCORE_SCALE
    q_pos = first_pos + jnp.arange(block_len)
    k_pos = jnp.arange(key_act.shape[0])
    q_doc = lax.dynamic_slice(doc_ids, (first_pos,), (block_len,))
    allowed = (k_pos[None, :] <= q_pos[:, None]) & (doc_ids[None, :] == q_doc[:, None])
    return scores, allowed[:, None, None, :]


def forward_lse(query, key_act, doc_ids):
    n_blocks = SLICES * SPLITS
    q_blocks = query.reshape(n_blocks, BLOCK_LEN, KV_HEADS, GROUP_SIZE, HEAD_DIM)
    firsts = PRE_LEN + jnp.arange(n_blocks) * BLOCK_LEN

    def block_lse(xs_blk):
        q_blk, first_pos = xs_blk
        scores, allowed = masked_scores(q_blk, key_act, doc_ids, first_pos)
        return jax.nn.logsumexp(jnp.where(allowed, scores, -1e30), axis=-1)

    return lax.map(block_lse, (q_blocks, firsts)).reshape(SLICES, SUB_LEN, Q_HEADS)


def setup_inputs(seed: int = 0, part: int = 0) -> dict:
    root_key = jax.random.key(seed)
    part_keys = jax.random.split(jax.random.fold_in(root_key, part), 5)
    doc_key = jax.random.key(seed + 17)
    starts = (jax.random.randint(doc_key, (PREFIX,), 0, DOC_MEAN) == 0) & (jnp.arange(PREFIX) > 0)
    doc_ids = jnp.cumsum(starts.astype(jnp.int32)).astype(jnp.int32)
    q_shape = (SLICES, SUB_LEN, Q_HEADS, HEAD_DIM)
    query = jax.random.normal(part_keys[0], q_shape, jnp.float32).astype(jnp.bfloat16)
    key_act = jax.random.normal(part_keys[1], (PREFIX, KV_HEADS, HEAD_DIM), jnp.float32).astype(jnp.bfloat16)
    value_act = jax.random.normal(part_keys[2], (PREFIX, KV_HEADS, HEAD_DIM), jnp.float32).astype(jnp.bfloat16)
    grad_dir = jax.random.normal(part_keys[3], q_shape, jnp.float32)
    out_noise = jax.random.normal(part_keys[4], q_shape, jnp.float32)
    out_grad = (GRAD_SCALE * grad_dir).astype(jnp.bfloat16)
    out_act = (0.125 * (grad_dir + out_noise)).astype(jnp.bfloat16)
    row_lse = forward_lse(query, key_act, doc_ids)
    return {'query': query, 'out_act': out_act, 'out_grad': out_grad, 'row_lse': row_lse, 'key_act': key_act, 'value_act': value_act, 'doc_ids': doc_ids}


def reference(query, out_act, out_grad, row_lse, key_act, value_act, doc_ids):
    n_blocks = SLICES * SPLITS
    blk_shape = (n_blocks, BLOCK_LEN, KV_HEADS, GROUP_SIZE, HEAD_DIM)
    key_f32 = key_act.astype(jnp.float32)
    value_f32 = value_act.astype(jnp.float32)
    xs_all = (query.reshape(blk_shape), out_act.reshape(blk_shape), out_grad.reshape(blk_shape), row_lse.reshape(n_blocks, BLOCK_LEN, KV_HEADS, GROUP_SIZE), PRE_LEN + jnp.arange(n_blocks) * BLOCK_LEN)

    def block_step(carry_in, xs_blk):
        dk_acc, dv_acc = carry_in
        q_blk, o_blk, do_blk, lse_blk, first_pos = xs_blk
        scores, allowed = masked_scores(q_blk, key_act, doc_ids, first_pos)
        p_full = jnp.where(allowed, jnp.exp(scores - lse_blk[..., None]), 0.0)
        p_half = p_full.astype(jnp.bfloat16).astype(jnp.float32)
        grad_f32 = do_blk.astype(jnp.float32)
        row_delta = jnp.sum(grad_f32 * o_blk.astype(jnp.float32), axis=-1)
        dv_acc = dv_acc + jnp.einsum('qhgk,qhgd->khd', p_half, grad_f32)
        d_prob = jnp.einsum('qhgd,khd->qhgk', grad_f32, value_f32)
        d_score = (p_full * (d_prob - row_delta[..., None])).astype(jnp.bfloat16).astype(jnp.float32)
        dq_blk = (jnp.einsum('qhgk,khd->qhgd', d_score, key_f32) * SCORE_SCALE).astype(jnp.bfloat16)
        dk_acc = dk_acc + jnp.einsum('qhgk,qhgd->khd', d_score, q_blk.astype(jnp.float32)) * SCORE_SCALE
        return (dk_acc, dv_acc), dq_blk

    zero_acc = jnp.zeros((PREFIX, KV_HEADS, HEAD_DIM), jnp.float32)
    (d_key, d_value), dq_blocks = lax.scan(block_step, (zero_acc, zero_acc), xs_all)
    return dq_blocks.reshape(SLICES, SUB_LEN, Q_HEADS, HEAD_DIM), d_key, d_value
```

```python
import functools

import jax
import jax.numpy as jnp
from jax import lax
from jax.experimental import pallas as pl
from jax.experimental.pallas import tpu as pltpu
from jax.sharding import PartitionSpec as P

LOG2E = 1.4426950408889634
KT = 256
VMEM = pltpu.VMEM


def attn_kernel(first_ref, last_ref, q_ref, do_ref, o_ref, lse_ref, start_ref, qpos_ref, k_ref, v_ref,
                dq_ref, dk_ref, dv_ref, kt_ref, delta_ref, *, n_tiles, rows, scale):
    d = q_ref.shape[1]
    n_kt = k_ref.shape[0] // KT
    nt = (((1,), (1,)), ((), ()))
    dk_ref[...] = jnp.zeros_like(dk_ref)
    dv_ref[...] = jnp.zeros_like(dv_ref)

    def transpose_keys(i, c):
        kt_ref[i] = k_ref[pl.ds(pl.multiple_of(i * KT, KT), KT), :].T
        return c

    lax.fori_loop(0, n_kt, transpose_keys, 0)

    def tile(t, c):
        r0 = pl.multiple_of(t * rows, rows)
        q = q_ref[pl.ds(r0, rows), :]
        do = do_ref[pl.ds(r0, rows), :]
        prod = do.astype(jnp.float32) * o_ref[pl.ds(r0, rows), :].astype(jnp.float32)
        delta = jnp.sum(prod.T, axis=0, keepdims=True)
        lse2 = lse_ref[t] * LOG2E
        start = start_ref[t]
        qpos = qpos_ref[t]

        def step(i, dqt):
            k0 = pl.multiple_of(i * KT, KT)
            k = k_ref[pl.ds(k0, KT), :]
            v = v_ref[pl.ds(k0, KT), :]
            s = lax.dot_general(k, q, nt, preferred_element_type=jnp.float32)
            kpos = lax.broadcasted_iota(jnp.int32, (KT, rows), 0) + k0
            allowed = (kpos >= start) & (kpos <= qpos)
            p = jnp.where(allowed, jnp.exp2(s * (scale * LOG2E) - lse2), 0.0)
            dv_ref[pl.ds(k0, KT), :] += jnp.dot(p.astype(jnp.bfloat16), do, preferred_element_type=jnp.float32)
            dp = lax.dot_general(v, do, nt, preferred_element_type=jnp.float32)
            ds = (p * (dp - delta)).astype(jnp.bfloat16)
            dk_ref[pl.ds(k0, KT), :] += jnp.dot(ds, q, preferred_element_type=jnp.float32)
            return dqt + jnp.dot(kt_ref[i], ds, preferred_element_type=jnp.float32)

        dqt = lax.fori_loop(first_ref[t], last_ref[t] + 1, step, jnp.zeros((d, rows), jnp.float32))
        dq_ref[pl.ds(r0, rows), :] = (dqt.T * scale).astype(jnp.bfloat16)
        return c

    lax.fori_loop(0, n_tiles, tile, 0)
    dk_ref[...] = dk_ref[...] * scale


def doc_starts(doc_ids):
    n = doc_ids.shape[0]
    ids = doc_ids.reshape(n // 128, 128)
    prev = jnp.concatenate([doc_ids[:1] - 1, doc_ids[:-1]]).reshape(n // 128, 128)
    pos = jnp.arange(n, dtype=jnp.int32).reshape(n // 128, 128)
    mark = jnp.where(ids != prev, pos, 0)
    lane = jnp.arange(128)
    inner = jnp.max(jnp.where(lane[None, None, :] <= lane[None, :, None], mark[:, None, :], 0), axis=-1)
    row_max = inner[:, -1]
    r = jnp.arange(n // 128)
    before = jnp.max(jnp.where(r[None, :] < r[:, None], row_max[None, :], 0), axis=-1)
    return jnp.maximum(inner, before[:, None]).reshape(n)


def solution(mesh):
    cp = mesh.shape['cp']
    q_spec = P(None, 'cp', 'tp', None)
    lse_spec = P(None, 'cp', 'tp')
    kv_spec = P('cp', 'tp', None)

    def local_backward(query, out_act, out_grad, row_lse, key_act, value_act, doc_ids):
        n_sub, loc, heads, d = query.shape
        n_keys = key_act.shape[0] * cp
        rows = loc * heads
        sub_len = loc * cp
        pre = n_keys - n_sub * sub_len
        scale = d ** -0.5
        me = lax.axis_index('cp')
        starts = doc_starts(doc_ids)
        tok = pre + me * loc + jnp.arange(n_sub, dtype=jnp.int32)[:, None] * sub_len + jnp.arange(loc, dtype=jnp.int32)[None, :]
        tok_start = lax.dynamic_slice(starts[pre:].reshape(n_sub, sub_len), (0, me * loc), (n_sub, loc))
        start_rows = jnp.repeat(tok_start, heads, axis=1).reshape(n_sub, 1, rows)
        pos_rows = jnp.repeat(tok, heads, axis=1).reshape(n_sub, 1, rows)
        first = tok_start[:, 0] // KT
        last = tok[:, -1] // KT
        kv = jnp.concatenate([key_act.reshape(-1, d), value_act.reshape(-1, d)], axis=1)
        kv = lax.all_gather(kv, 'cp', axis=0, tiled=True)
        keys, values = kv[:, :d], kv[:, d:]
        vm = pl.BlockSpec(memory_space=VMEM)
        sm = pl.BlockSpec(memory_space=pltpu.SMEM)
        dq, dk, dv = pl.pallas_call(
            functools.partial(attn_kernel, n_tiles=n_sub, rows=rows, scale=scale),
            out_shape=(jax.ShapeDtypeStruct((n_sub * rows, d), jnp.bfloat16),
                       jax.ShapeDtypeStruct((n_keys, d), jnp.float32),
                       jax.ShapeDtypeStruct((n_keys, d), jnp.float32)),
            in_specs=[sm, sm] + [vm] * 8,
            out_specs=(vm, vm, vm),
            scratch_shapes=[VMEM((n_keys // KT, d, KT), jnp.bfloat16), VMEM((8, rows), jnp.float32)],
            compiler_params=pltpu.CompilerParams(vmem_limit_bytes=50 * 1024 * 1024),
            name='attn_bwd',
        )(first, last, query.reshape(-1, d), out_grad.reshape(-1, d), out_act.reshape(-1, d),
          row_lse.reshape(n_sub, 1, rows), start_rows, pos_rows, keys, values)
        dkv = lax.psum_scatter(jnp.concatenate([dk, dv], axis=1), 'cp', scatter_dimension=0, tiled=True)
        return (dq.reshape(query.shape), dkv[:, :d].reshape(key_act.shape), dkv[:, d:].reshape(value_act.shape))

    return jax.shard_map(local_backward, mesh=mesh, in_specs=(q_spec, q_spec, q_spec, lse_spec, kv_spec, kv_spec, P()), out_specs=(q_spec, kv_spec, kv_spec), check_vma=False)
```

```python
import functools

import jax
import jax.numpy as jnp
from jax import lax
from jax.experimental import pallas as pl
from jax.experimental.pallas import tpu as pltpu
from jax.sharding import PartitionSpec as P

LOG2E = 1.4426950408889634
NT = (((1,), (1,)), ((), ()))
MESH = pl.DeviceIdType.MESH
VMEM, SMEM = pltpu.VMEM, pltpu.SMEM
HIGHEST = lax.Precision.HIGHEST
KT = 256
UNROLL = 4


def flip(me, bit):
    return me + bit - 2 * bit * lax.rem(me // bit, 2)


def gather_kernel(k_ref, v_ref, q_ref, do_ref, o_ref, lse_ref, ids_ref,
                  kx_ref, vx_ref, ky_ref, vy_ref, kd_ref, vd_ref, q2_ref, do2_ref, lse2_ref, delta_ref, start_ref, first_ref,
                  o2_ref, lraw_ref, mark_ref, send_sem, recv_sem, *, pre, sub_len, loc, heads):
    me = lax.axis_index('cp')
    core = lax.rem(me, 2)
    nx, ny, nc = flip(me, 2), flip(me, 4), flip(me, 1)
    barrier = pltpu.get_barrier_semaphore()
    for other in (nx, ny, nc):
        pl.semaphore_signal(barrier, inc=1, device_id={'cp': other}, device_id_type=MESH)
    pl.semaphore_wait(barrier, 3)

    def send(i, src, dst, to):
        copy = pltpu.make_async_remote_copy(src_ref=src, dst_ref=dst, send_sem=send_sem.at[i], recv_sem=recv_sem.at[i],
                                            device_id={'cp': to}, device_id_type=MESH)
        copy.start()
        return copy

    c_kx = send(0, k_ref, kx_ref, nx)
    c_vy = send(1, v_ref, vy_ref, ny)
    c_o = send(4, o_ref, o2_ref.at[core], nc)
    c_do = send(5, do_ref, do2_ref.at[core], nc)
    c_lse = send(6, lse_ref, lraw_ref.at[core], nc)
    c_q = send(7, q_ref, q2_ref.at[core], nc)
    c_vx = send(2, v_ref, vx_ref, nx)
    c_ky = send(3, k_ref, ky_ref, ny)

    q2_ref[core] = q_ref[...]
    do2_ref[core] = do_ref[...]
    lraw_ref[core] = lse_ref[...]

    n_rows = ids_ref.shape[0]
    n_sub = lraw_ref.shape[1]
    pad = mark_ref.shape[0]
    mark_ref[...] = jnp.zeros_like(mark_ref)
    mark_ref[0:n_rows, :] = ids_ref[...]
    ids = mark_ref[...]
    lane = lax.broadcasted_iota(jnp.int32, (pad, 128), 1)
    row = lax.broadcasted_iota(jnp.int32, (pad, 128), 0)
    prev = pltpu.roll(ids, 1, axis=1)
    prev = jnp.where(lane == 0, pltpu.roll(prev, 1, axis=0), prev)
    acc = jnp.where(ids != prev, row * 128 + lane, 0)
    for sh in (1, 2, 4, 8, 16, 32, 64):
        acc = jnp.maximum(acc, jnp.where(lane >= sh, pltpu.roll(acc, sh, axis=1), 0))
    carry = jnp.max(acc, axis=1, keepdims=True) + jnp.zeros((pad, 128), jnp.int32)
    carry = jnp.where(row >= 1, pltpu.roll(carry, 1, axis=0), 0)
    sh = 1
    while sh < pad:
        carry = jnp.maximum(carry, jnp.where(row >= sh, pltpu.roll(carry, sh, axis=0), 0))
        sh *= 2
    starts = jnp.maximum(acc, carry).astype(jnp.float32)

    def hdot(a, b, dims=None):
        dims = (((1,), (0,)), ((), ())) if dims is None else dims
        return lax.dot_general(a, b, dims, precision=HIGHEST, preferred_element_type=jnp.float32)

    per = sub_len // 128
    off = (me // 2) * 2 * loc
    r_sub = lax.broadcasted_iota(jnp.int32, (n_sub, pad), 0)
    r_row = lax.broadcasted_iota(jnp.int32, (n_sub, pad), 1)
    pick = jnp.where(r_row == pre // 128 + per * r_sub + off // 128, 1.0, 0.0)
    sub_starts = hdot(pick, starts)
    src = lax.broadcasted_iota(jnp.int32, (128, 128), 0)
    dst = lax.broadcasted_iota(jnp.int32, (128, 128), 1)
    for e in range(2):
        spread = jnp.where(src == lax.rem(off, 128) + e * loc + dst // heads, 1.0, 0.0)
        rows_start = hdot(sub_starts, spread)
        start_ref[e] = rows_start.astype(jnp.int32)
        if e == 0:
            head = jnp.where(lax.broadcasted_iota(jnp.int32, (8, 128), 1) == 0, 1.0, 0.0)
            first_ref[...] = hdot(head, rows_start, NT).astype(jnp.int32)

    def delta_of(e, o_part):
        def body(t, c):
            r0 = pl.multiple_of(t * 128, 128)
            prod = do2_ref[e, pl.ds(r0, 128), :].astype(jnp.float32) * o_part[pl.ds(r0, 128), :].astype(jnp.float32)
            delta_ref[e, pl.ds(t, 1), :] = jnp.sum(prod.T, axis=0, keepdims=True)
            return c
        lax.fori_loop(0, n_sub, body, 0)

    delta_of(core, o_ref)
    c_o.wait_recv()
    c_do.wait_recv()
    delta_of(1 - core, o2_ref.at[1 - core])
    c_kx.wait_recv()
    c_kd = send(8, kx_ref, kd_ref, ny)
    c_vy.wait_recv()
    c_vd = send(9, vy_ref, vd_ref, nx)
    c_lse.wait_recv()
    tok = lax.broadcasted_iota(jnp.int32, (loc, 128), 0)
    tok_lane = lax.broadcasted_iota(jnp.int32, (loc, 128), 1)
    tok_spread = jnp.where(tok == tok_lane // heads, 1.0, 0.0)
    head_of = lax.broadcasted_iota(jnp.int32, (n_sub * heads, 128), 0)
    head_lane = lax.broadcasted_iota(jnp.int32, (n_sub * heads, 128), 1)
    own_head = lax.rem(head_of, heads) == lax.rem(head_lane, heads)
    g_sub = lax.broadcasted_iota(jnp.int32, (n_sub, n_sub * heads), 0)
    g_row = lax.broadcasted_iota(jnp.int32, (n_sub, n_sub * heads), 1)
    group = jnp.where(g_row // heads == g_sub, 1.0, 0.0)
    for e in range(2):
        wide = hdot(lraw_ref[e].reshape(n_sub * heads, loc), tok_spread)
        lse2_ref[e] = hdot(group, jnp.where(own_head, wide, 0.0)) * LOG2E
    c_q.wait_recv()
    c_vx.wait_recv()
    c_ky.wait_recv()
    c_kd.wait_recv()
    c_vd.wait_recv()
    for copy in (c_kx, c_vy, c_vx, c_ky, c_o, c_do, c_lse, c_q, c_kd, c_vd):
        copy.wait_send()


def attn_kernel(*refs, owner_bits, has_dq, finish, scale, pre, sub_len, loc, heads):
    n_in = 9 if has_dq else 8
    first_ref, q_ref, do_ref, lse_ref, delta_ref, start_ref, k_ref, v_ref = refs[:8]
    if finish:
        own_ref, other_ref, dk_ref, dv_ref, dq_ref = refs[n_in:n_in + 5]
        it_t, it_k, it_lo = refs[n_in + 5:]
    else:
        dq_ref, dk_ref, dv_ref = refs[n_in:n_in + 3]
        it_t, it_k, it_lo = refs[n_in + 3:]
    me = lax.axis_index('cp')
    core = lax.rem(me, 2)
    owner = me
    for bit in owner_bits:
        owner = flip(owner, bit)
    blk = k_ref.shape[0]
    n_sub, half = lse_ref.shape[1], lse_ref.shape[2]
    rows = 2 * half
    blo = owner * blk
    pos0 = pre + (me // 2) * 2 * loc
    dk_ref[...] = jnp.zeros_like(dk_ref)
    dv_ref[...] = jnp.zeros_like(dv_ref)
    if finish:
        dq_ref[...] = refs[8][...]
    elif has_dq:
        dq_ref[...] = refs[8][...]
    else:
        dq_ref[...] = jnp.zeros_like(dq_ref)

    def add_tile(t, n):
        lo = jnp.maximum(first_ref[0, t], blo)
        hi = jnp.minimum(pos0 + t * sub_len + 2 * loc - 1, blo + blk - 1)
        off = (lo - blo) // 16 * 16
        cnt = jnp.where(hi >= lo, (hi - blo - off) // KT + 1, 0)

        def add_item(i, m):
            it_t[m] = t
            it_k[m] = jnp.minimum(off + i * KT, blk - KT)
            it_lo[m] = blo + off + i * KT
            return m + 1

        return lax.fori_loop(0, cnt, add_item, n)

    n_items = lax.fori_loop(0, n_sub, add_tile, 0)
    for u in range(UNROLL - 1):
        it_t[n_items + u] = 0
        it_k[n_items + u] = 0
        it_lo[n_items + u] = 1 << 30

    def two(ref, t):
        return jnp.concatenate([ref[0, pl.ds(t, 1), :], ref[1, pl.ds(t, 1), :]], axis=1)

    lane = lax.broadcasted_iota(jnp.int32, (1, rows), 1)

    def body(w, c):
        st = []
        for u in range(UNROLL):
            m = w * UNROLL + u
            t = it_t[m]
            k0 = pl.multiple_of(it_k[m], 16)
            r0 = pl.multiple_of(t * half, half)
            k = k_ref[pl.ds(k0, KT), :]
            v = v_ref[pl.ds(k0, KT), :]
            q = jnp.concatenate([q_ref[0, pl.ds(r0, half), :], q_ref[1, pl.ds(r0, half), :]], axis=0)
            do = jnp.concatenate([do_ref[0, pl.ds(r0, half), :], do_ref[1, pl.ds(r0, half), :]], axis=0)
            s = lax.dot_general(k, q, NT, preferred_element_type=jnp.float32)
            dp = lax.dot_general(v, do, NT, preferred_element_type=jnp.float32)
            st.append((m, t, k0, k, q, do, s, dp))
        mid = []
        for u in range(UNROLL):
            m, t, k0, k, q, do, s, dp = st[u]
            lo = jnp.maximum(two(start_ref, t), it_lo[m])
            qpos = lane // heads + (pos0 + t * sub_len)
            kpos = lax.broadcasted_iota(jnp.int32, (KT, rows), 0) + (k0 + blo)
            allowed = (kpos >= lo) & (kpos <= qpos)
            p = jnp.where(allowed, jnp.exp2(s * (scale * LOG2E) - two(lse_ref, t)), 0.0)
            ds = (p * (dp - two(delta_ref, t))).astype(jnp.bfloat16)
            mid.append((p.astype(jnp.bfloat16), ds))
        for u in range(UNROLL):
            m, t, k0, k, q, do, s, dp = st[u]
            p, ds = mid[u]
            dv_ref[pl.ds(k0, KT), :] += jnp.dot(p, do, preferred_element_type=jnp.float32)
            dk_ref[pl.ds(k0, KT), :] += jnp.dot(ds, q, preferred_element_type=jnp.float32)
            dq_ref[t] += jnp.dot(k.T, ds, preferred_element_type=jnp.float32)
        return c

    lax.fori_loop(0, (n_items + UNROLL - 1) // UNROLL, body, 0)
    if finish:
        mine = pl.multiple_of(core * half, half)
        theirs = pl.multiple_of((1 - core) * half, half)

        def put(t, c):
            r0 = pl.multiple_of(t * half, half)
            own_ref[pl.ds(r0, half), :] = dq_ref[t, :, pl.ds(mine, half)].T
            other_ref[pl.ds(r0, half), :] = dq_ref[t, :, pl.ds(theirs, half)].T
            return c

        lax.fori_loop(0, n_sub, put, 0)


def solution(mesh):
    cp = mesh.shape['cp']
    q_spec = P(None, 'cp', 'tp', None)
    lse_spec = P(None, 'cp', 'tp')
    kv_spec = P('cp', 'tp', None)

    def swap(x, bits):
        return lax.ppermute(x, 'cp', [(i, i ^ bits) for i in range(cp)])

    def local_backward(query, out_act, out_grad, row_lse, key_act, value_act, doc_ids):
        n_sub, loc, heads, d = query.shape
        blk = key_act.shape[0]
        n_keys = blk * cp
        half = loc * heads
        sub_len = loc * cp
        pre = n_keys - n_sub * sub_len
        scale = d ** -0.5
        f32, bf16, i32 = jnp.float32, jnp.bfloat16, jnp.int32
        dims = dict(pre=pre, sub_len=sub_len, loc=loc, heads=heads)
        vm = pl.BlockSpec(memory_space=VMEM)
        sm = pl.BlockSpec(memory_space=SMEM)
        sds = jax.ShapeDtypeStruct
        k_own, v_own = key_act.reshape(blk, d), value_act.reshape(blk, d)
        pad = (n_keys // 128 + 7) // 8 * 8
        kx, vx, ky, vy, kd, vd, q2, do2, lse2, delta, start, first = pl.pallas_call(
            functools.partial(gather_kernel, **dims),
            out_shape=tuple([sds((blk, d), bf16)] * 6 + [sds((2, n_sub * half, d), bf16)] * 2
                            + [sds((2, n_sub, half), f32)] * 2 + [sds((2, n_sub, half), i32), sds((8, n_sub), i32)]),
            in_specs=[vm] * 7, out_specs=(vm,) * 12,
            scratch_shapes=[VMEM((2, n_sub * half, d), bf16), VMEM((2, n_sub, heads, loc), f32), VMEM((pad, 128), i32),
                            pltpu.SemaphoreType.DMA((10,)), pltpu.SemaphoreType.DMA((10,))],
            compiler_params=pltpu.CompilerParams(collective_id=0, has_side_effects=True, vmem_limit_bytes=24 * 2 ** 20),
            name='gather_kv',
        )(k_own, v_own, query.reshape(-1, d), out_grad.reshape(-1, d), out_act.reshape(-1, d),
          row_lse.transpose(0, 2, 1), doc_ids.reshape(n_keys // 128, 128))

        cap = n_sub * (-(-blk // KT) + 1) + UNROLL
        items = [SMEM((cap,), i32)] * 3
        acc = sds((n_sub, d, 2 * half), f32)
        kv_out = sds((blk, d), f32)
        dq_out = sds((n_sub * half, d), f32)
        cost = pl.CostEstimate(flops=2 * 10 ** 9, bytes_accessed=10 ** 7, transcendentals=10 ** 6)

        def attend(bits, k, v, dq=None, finish=False):
            ins = [first, q2, do2, lse2, delta, start, k, v] + ([dq] if dq is not None else [])
            outs = (dq_out, dq_out, kv_out, kv_out) if finish else (acc, kv_out, kv_out)
            return pl.pallas_call(
                functools.partial(attn_kernel, owner_bits=bits, has_dq=dq is not None, finish=finish, scale=scale, **dims),
                out_shape=outs, in_specs=[sm] + [vm] * (len(ins) - 1), out_specs=(vm,) * len(outs),
                scratch_shapes=([VMEM((n_sub, d, 2 * half), f32)] if finish else []) + items,
                compiler_params=pltpu.CompilerParams(vmem_limit_bytes=28 * 2 ** 20),
                cost_estimate=cost, name='attn_bwd')(*ins)

        dq, dk_d, dv_d = attend((2, 4), kd, vd)
        got_ky = swap(dk_d, 2)
        got_vx = swap(dv_d, 4)
        dq, dk_x, dv_x = attend((2,), kx, vx, dq)
        got_ko = swap(dk_x, 2)
        dq, dk_y, dv_y = attend((4,), ky, vy, dq)
        got_vo = swap(dv_y, 4)
        dq_own, dq_other, dk_o, dv_o = attend((), k_own, v_own, dq, finish=True)
        last_k = swap(dk_y + got_ky, 4)
        last_v = swap(dv_x + got_vx, 2)
        got_dq = swap(dq_other, 1)
        d_query = ((dq_own + got_dq) * scale).astype(bf16)
        d_key = (dk_o + got_ko + last_k) * scale
        d_value = dv_o + got_vo + last_v
        return d_query.reshape(query.shape), d_key.reshape(key_act.shape), d_value.reshape(value_act.shape)

    return jax.shard_map(local_backward, mesh=mesh, in_specs=(q_spec, q_spec, q_spec, lse_spec, kv_spec, kv_spec, P()), out_specs=(q_spec, kv_spec, kv_spec), check_vma=False)
```

```python
import functools

import jax
import jax.numpy as jnp
from jax import lax
from jax.experimental import pallas as pl
from jax.experimental.pallas import tpu as pltpu
from jax.sharding import PartitionSpec as P


LOG2E = 1.4426950408889634
NT = (((1,), (1,)), ((), ()))
MESH = pl.DeviceIdType.MESH
VMEM, SMEM = pltpu.VMEM, pltpu.SMEM
HIGHEST = lax.Precision.HIGHEST
KT = 256
UNROLL = 4


def flip(me, bit):
    return me + bit - 2 * bit * lax.rem(me // bit, 2)


def gather_kernel(k_ref, v_ref, q_ref, do_ref, o_ref, lse_ref, ids_ref,
                  kx_ref, vx_ref, ky_ref, vy_ref, kd_ref, vd_ref, q2_ref, do2_ref, lse2_ref, delta_ref, start_ref, first_ref,
                  o2_ref, lraw_ref, mark_ref, send_sem, recv_sem, load_sem, *, pre, sub_len, loc, heads):
    me = lax.axis_index('cp')
    core = lax.rem(me, 2)
    nx, ny, nc = flip(me, 2), flip(me, 4), flip(me, 1)
    barrier = pltpu.get_barrier_semaphore()
    for other in (nx, ny, nc):
        pl.semaphore_signal(barrier, inc=1, device_id={'cp': other}, device_id_type=MESH)
    pl.semaphore_wait(barrier, 3)

    def send(i, src, dst, to):
        copy = pltpu.make_async_remote_copy(src_ref=src, dst_ref=dst, send_sem=send_sem.at[i], recv_sem=recv_sem.at[i],
                                            device_id={'cp': to}, device_id_type=MESH)
        copy.start()
        return copy

    c_kx = send(0, k_ref, kx_ref, nx)
    c_vy = send(1, v_ref, vy_ref, ny)
    c_o = send(4, o_ref, o2_ref.at[core], nc)
    c_do = send(5, do_ref, do2_ref.at[core], nc)
    c_lse = send(6, lse_ref, lraw_ref.at[core], nc)
    c_q = send(7, q_ref, q2_ref.at[core], nc)
    c_vx = send(2, v_ref, vx_ref, nx)
    c_ky = send(3, k_ref, ky_ref, ny)

    loads = [pltpu.make_async_copy(s, r.at[core], load_sem.at[i])
             for i, (s, r) in enumerate([(do_ref, do2_ref), (o_ref, o2_ref), (lse_ref, lraw_ref), (q_ref, q2_ref)])]
    for load in loads:
        load.start()

    n_rows = ids_ref.shape[0]
    n_sub = lraw_ref.shape[1]
    pad = mark_ref.shape[0]
    mark_ref[...] = jnp.zeros_like(mark_ref)
    mark_ref[0:n_rows, :] = ids_ref[...]
    ids = mark_ref[...]
    lane = lax.broadcasted_iota(jnp.int32, (pad, 128), 1)
    row = lax.broadcasted_iota(jnp.int32, (pad, 128), 0)
    prev = pltpu.roll(ids, 1, axis=1)
    prev = jnp.where(lane == 0, pltpu.roll(prev, 1, axis=0), prev)
    acc = jnp.where(ids != prev, row * 128 + lane, 0)
    for sh in (1, 2, 4, 8, 16, 32, 64):
        acc = jnp.maximum(acc, jnp.where(lane >= sh, pltpu.roll(acc, sh, axis=1), 0))
    carry = jnp.max(acc, axis=1, keepdims=True) + jnp.zeros((pad, 128), jnp.int32)
    carry = jnp.where(row >= 1, pltpu.roll(carry, 1, axis=0), 0)
    sh = 1
    while sh < pad:
        carry = jnp.maximum(carry, jnp.where(row >= sh, pltpu.roll(carry, sh, axis=0), 0))
        sh *= 2
    starts = jnp.maximum(acc, carry).astype(jnp.float32)

    def hdot(a, b, dims=None):
        dims = (((1,), (0,)), ((), ())) if dims is None else dims
        return lax.dot_general(a, b, dims, precision=HIGHEST, preferred_element_type=jnp.float32)

    per = sub_len // 128
    off = (me // 2) * 2 * loc
    r_sub = lax.broadcasted_iota(jnp.int32, (n_sub, pad), 0)
    r_row = lax.broadcasted_iota(jnp.int32, (n_sub, pad), 1)
    pick = jnp.where(r_row == pre // 128 + per * r_sub + off // 128, 1.0, 0.0)
    sub_starts = hdot(pick, starts)
    src = lax.broadcasted_iota(jnp.int32, (128, 128), 0)
    dst = lax.broadcasted_iota(jnp.int32, (128, 128), 1)
    for e in range(2):
        spread = jnp.where(src == lax.rem(off, 128) + e * loc + dst // heads, 1.0, 0.0)
        rows_start = hdot(sub_starts, spread)
        start_ref[e] = rows_start.astype(jnp.int32)
        if e == 0:
            head = jnp.where(lax.broadcasted_iota(jnp.int32, (8, 128), 1) == 0, 1.0, 0.0)
            first_ref[...] = hdot(head, rows_start, NT).astype(jnp.int32)

    def delta_of(e, o_part):
        def body(t, c):
            r0 = pl.multiple_of(t * 128, 128)
            prod = do2_ref[e, pl.ds(r0, 128), :].astype(jnp.float32) * o_part[pl.ds(r0, 128), :].astype(jnp.float32)
            delta_ref[e, pl.ds(t, 1), :] = jnp.sum(prod.T, axis=0, keepdims=True)
            return c

        lax.fori_loop(0, n_sub, body, 0)

    for load in loads:
        load.wait()
    delta_of(core, o2_ref.at[core])
    c_o.wait_recv()
    c_do.wait_recv()
    delta_of(1 - core, o2_ref.at[1 - core])
    c_kx.wait_recv()
    c_kd = send(8, kx_ref, kd_ref, ny)
    c_vy.wait_recv()
    c_vd = send(9, vy_ref, vd_ref, nx)
    c_lse.wait_recv()
    tok = lax.broadcasted_iota(jnp.int32, (loc, 128), 0)
    tok_lane = lax.broadcasted_iota(jnp.int32, (loc, 128), 1)
    tok_spread = jnp.where(tok == tok_lane // heads, 1.0, 0.0)
    head_of = lax.broadcasted_iota(jnp.int32, (n_sub * heads, 128), 0)
    head_lane = lax.broadcasted_iota(jnp.int32, (n_sub * heads, 128), 1)
    own_head = lax.rem(head_of, heads) == lax.rem(head_lane, heads)
    g_sub = lax.broadcasted_iota(jnp.int32, (n_sub, n_sub * heads), 0)
    g_row = lax.broadcasted_iota(jnp.int32, (n_sub, n_sub * heads), 1)
    group = jnp.where(g_row // heads == g_sub, 1.0, 0.0)
    for e in range(2):
        wide = hdot(lraw_ref[e].reshape(n_sub * heads, loc), tok_spread)
        lse2_ref[e] = hdot(group, jnp.where(own_head, wide, 0.0)) * LOG2E
    c_q.wait_recv()
    c_vx.wait_recv()
    c_ky.wait_recv()
    c_kd.wait_recv()
    c_vd.wait_recv()
    for copy in (c_kx, c_vy, c_vx, c_ky, c_o, c_do, c_lse, c_q, c_kd, c_vd):
        copy.wait_send()


def attn_kernel(*refs, owner_bits, has_dq, finish, scale, pre, sub_len, loc, heads):
    n_in = 9 if has_dq else 8
    first_ref, q_ref, do_ref, lse_ref, delta_ref, start_ref, k_ref, v_ref = refs[:8]
    if finish:
        own_ref, other_ref, dk_ref, dv_ref, dq_ref = refs[n_in:n_in + 5]
        it_t, it_k, it_lo = refs[n_in + 5:]
    else:
        dq_ref, dk_ref, dv_ref = refs[n_in:n_in + 3]
        it_t, it_k, it_lo = refs[n_in + 3:]
    me = lax.axis_index('cp')
    core = lax.rem(me, 2)
    owner = me
    for bit in owner_bits:
        owner = flip(owner, bit)
    blk = k_ref.shape[0]
    n_sub, half = lse_ref.shape[1], lse_ref.shape[2]
    rows = 2 * half
    blo = owner * blk
    pos0 = pre + (me // 2) * 2 * loc
    dk_ref[...] = jnp.zeros_like(dk_ref)
    dv_ref[...] = jnp.zeros_like(dv_ref)
    if finish:
        dq_ref[...] = refs[8][...]
    elif has_dq:
        dq_ref[...] = refs[8][...]
    else:
        dq_ref[...] = jnp.zeros_like(dq_ref)

    def add_tile(t, n):
        lo = jnp.maximum(first_ref[0, t], blo)
        hi = jnp.minimum(pos0 + t * sub_len + 2 * loc - 1, blo + blk - 1)
        off = (lo - blo) // 16 * 16
        cnt = jnp.where(hi >= lo, (hi - blo - off) // KT + 1, 0)

        def add_item(i, m):
            it_t[m] = t
            it_k[m] = jnp.minimum(off + i * KT, blk - KT)
            it_lo[m] = blo + off + i * KT
            return m + 1

        return lax.fori_loop(0, cnt, add_item, n)

    n_items = lax.fori_loop(0, n_sub, add_tile, 0)
    for u in range(UNROLL - 1):
        it_t[n_items + u] = 0
        it_k[n_items + u] = 0
        it_lo[n_items + u] = 1 << 30

    def two(ref, t):
        return jnp.concatenate([ref[0, pl.ds(t, 1), :], ref[1, pl.ds(t, 1), :]], axis=1)

    lane = lax.broadcasted_iota(jnp.int32, (1, rows), 1)

    def body(w, c):
        st = []
        for u in range(UNROLL):
            m = w * UNROLL + u
            t = it_t[m]
            k0 = pl.multiple_of(it_k[m], 16)
            r0 = pl.multiple_of(t * half, half)
            k = k_ref[pl.ds(k0, KT), :]
            v = v_ref[pl.ds(k0, KT), :]
            q = jnp.concatenate([q_ref[0, pl.ds(r0, half), :], q_ref[1, pl.ds(r0, half), :]], axis=0)
            do = jnp.concatenate([do_ref[0, pl.ds(r0, half), :], do_ref[1, pl.ds(r0, half), :]], axis=0)
            s = lax.dot_general(k, q, NT, preferred_element_type=jnp.float32)
            dp = lax.dot_general(v, do, NT, preferred_element_type=jnp.float32)
            st.append((m, t, k0, k, q, do, s, dp))
        mid = []
        for u in range(UNROLL):
            m, t, k0, k, q, do, s, dp = st[u]
            lo = jnp.maximum(two(start_ref, t), it_lo[m])
            qpos = lane // heads + (pos0 + t * sub_len)
            kpos = lax.broadcasted_iota(jnp.int32, (KT, rows), 0) + (k0 + blo)
            allowed = (kpos >= lo) & (kpos <= qpos)
            p = jnp.where(allowed, jnp.exp2(s * (scale * LOG2E) - two(lse_ref, t)), 0.0)
            ds = (p * (dp - two(delta_ref, t))).astype(jnp.bfloat16)
            mid.append((p.astype(jnp.bfloat16), ds))
        for u in range(UNROLL):
            m, t, k0, k, q, do, s, dp = st[u]
            p, ds = mid[u]
            dv_ref[pl.ds(k0, KT), :] += jnp.dot(p, do, preferred_element_type=jnp.float32)
            dk_ref[pl.ds(k0, KT), :] += jnp.dot(ds, q, preferred_element_type=jnp.float32)
            dq_ref[t] += jnp.dot(k.T, ds, preferred_element_type=jnp.float32)
        return c

    lax.fori_loop(0, (n_items + UNROLL - 1) // UNROLL, body, 0)
    if finish:
        mine = pl.multiple_of(core * half, half)
        theirs = pl.multiple_of((1 - core) * half, half)

        def put(t, c):
            r0 = pl.multiple_of(t * half, half)
            own_ref[pl.ds(r0, half), :] = dq_ref[t, :, pl.ds(mine, half)].T
            other_ref[pl.ds(r0, half), :] = dq_ref[t, :, pl.ds(theirs, half)].T
            return c

        lax.fori_loop(0, n_sub, put, 0)


def solution(mesh):
    cp = mesh.shape['cp']
    q_spec = P(None, 'cp', 'tp', None)
    lse_spec = P(None, 'cp', 'tp')
    kv_spec = P('cp', 'tp', None)

    def swap(x, bits):
        return lax.ppermute(x, 'cp', [(i, i ^ bits) for i in range(cp)])

    def local_backward(query, out_act, out_grad, row_lse, key_act, value_act, doc_ids):
        n_sub, loc, heads, d = query.shape
        blk = key_act.shape[0]
        n_keys = blk * cp
        half = loc * heads
        sub_len = loc * cp
        pre = n_keys - n_sub * sub_len
        scale = d ** -0.5
        f32, bf16, i32 = jnp.float32, jnp.bfloat16, jnp.int32
        dims = dict(pre=pre, sub_len=sub_len, loc=loc, heads=heads)
        vm = pl.BlockSpec(memory_space=VMEM)
        sm = pl.BlockSpec(memory_space=SMEM)
        hbm = pl.BlockSpec(memory_space=pltpu.HBM)
        sds = jax.ShapeDtypeStruct
        k_own, v_own = key_act.reshape(blk, d), value_act.reshape(blk, d)
        pad = (n_keys // 128 + 7) // 8 * 8
        kx, vx, ky, vy, kd, vd, q2, do2, lse2, delta, start, first = pl.pallas_call(
            functools.partial(gather_kernel, **dims),
            out_shape=tuple([sds((blk, d), bf16)] * 6 + [sds((2, n_sub * half, d), bf16)] * 2
                            + [sds((2, n_sub, half), f32)] * 2 + [sds((2, n_sub, half), i32), sds((8, n_sub), i32)]),
            in_specs=[hbm] * 6 + [vm], out_specs=(vm,) * 12,
            scratch_shapes=[VMEM((2, n_sub * half, d), bf16), VMEM((2, n_sub, heads, loc), f32), VMEM((pad, 128), i32),
                            pltpu.SemaphoreType.DMA((10,)), pltpu.SemaphoreType.DMA((10,)), pltpu.SemaphoreType.DMA((4,))],
            compiler_params=pltpu.CompilerParams(collective_id=0, has_side_effects=True, vmem_limit_bytes=24 * 2 ** 20),
            name='gather_kv',
        )(k_own, v_own, query.reshape(-1, d), out_grad.reshape(-1, d), out_act.reshape(-1, d),
          row_lse.transpose(0, 2, 1), doc_ids.reshape(n_keys // 128, 128))

        cap = n_sub * (-(-blk // KT) + 1) + UNROLL
        items = [SMEM((cap,), i32)] * 3
        acc = sds((n_sub, d, 2 * half), f32)
        kv_out = sds((blk, d), f32)
        dq_out = sds((n_sub * half, d), f32)
        cost = pl.CostEstimate(flops=2 * 10 ** 9, bytes_accessed=10 ** 7, transcendentals=10 ** 6)

        def attend(bits, k, v, dq=None, finish=False):
            ins = [first, q2, do2, lse2, delta, start, k, v] + ([dq] if dq is not None else [])
            outs = (dq_out, dq_out, kv_out, kv_out) if finish else (acc, kv_out, kv_out)
            return pl.pallas_call(
                functools.partial(attn_kernel, owner_bits=bits, has_dq=dq is not None, finish=finish, scale=scale, **dims),
                out_shape=outs, in_specs=[sm] + [vm] * (len(ins) - 1), out_specs=(vm,) * len(outs),
                scratch_shapes=([VMEM((n_sub, d, 2 * half), f32)] if finish else []) + items,
                compiler_params=pltpu.CompilerParams(vmem_limit_bytes=28 * 2 ** 20),
                cost_estimate=cost, name='attn_bwd')(*ins)

        def run(bits, k, v, dq=None, finish=False):
            return attend(bits, k, v, dq, finish)

        dq, dk_d, dv_d = run((2, 4), kd, vd)
        got_ky = swap(dk_d, 2)
        got_vx = swap(dv_d, 4)
        dq, dk_x, dv_x = run((2,), kx, vx, dq)
        got_ko = swap(dk_x, 2)
        dq, dk_y, dv_y = run((4,), ky, vy, dq)
        got_vo = swap(dv_y, 4)
        dq_own, dq_other, dk_o, dv_o = run((), k_own, v_own, dq, finish=True)
        last_k = swap(dk_y + got_ky, 4)
        last_v = swap(dv_x + got_vx, 2)
        got_dq = swap(dq_other, 1)
        d_query = ((dq_own + got_dq) * scale).astype(bf16)
        d_key = (dk_o + got_ko + last_k) * scale
        d_value = dv_o + got_vo + last_v
        return d_query.reshape(query.shape), d_key.reshape(key_act.shape), d_value.reshape(value_act.shape)

    return jax.shard_map(local_backward, mesh=mesh, in_specs=(q_spec, q_spec, q_spec, lse_spec, kv_spec, kv_spec, P()), out_specs=(q_spec, kv_spec, kv_spec), check_vma=False)
```

```python
import functools

import jax
import jax.numpy as jnp
from jax import lax
from jax.experimental import pallas as pl
from jax.experimental.pallas import tpu as pltpu
from jax.sharding import PartitionSpec as P


LOG2E = 1.4426950408889634
NT = (((1,), (1,)), ((), ()))
MESH = pl.DeviceIdType.MESH
VMEM, SMEM = pltpu.VMEM, pltpu.SMEM
HIGHEST = lax.Precision.HIGHEST
KT = 256
UNROLL = 4


def flip(me, bit):
    return me + bit - 2 * bit * lax.rem(me // bit, 2)


def gather_kernel(k_ref, v_ref, q_ref, do_ref, o_ref, lse_ref, ids_ref,
                  kx_ref, vx_ref, ky_ref, vy_ref, kd_ref, vd_ref, q2_ref, do2_ref, lse2_ref, delta_ref, start_ref, first_ref,
                  o2_ref, lraw_ref, mark_ref, send_sem, recv_sem, load_sem, *, pre, sub_len, loc, heads):
    me = lax.axis_index('cp')
    core = lax.rem(me, 2)
    nx, ny, nc = flip(me, 2), flip(me, 4), flip(me, 1)
    barrier = pltpu.get_barrier_semaphore()
    for other in (nx, ny, nc):
        pl.semaphore_signal(barrier, inc=1, device_id={'cp': other}, device_id_type=MESH)
    pl.semaphore_wait(barrier, 3)

    def send(i, src, dst, to):
        copy = pltpu.make_async_remote_copy(src_ref=src, dst_ref=dst, send_sem=send_sem.at[i], recv_sem=recv_sem.at[i],
                                            device_id={'cp': to}, device_id_type=MESH)
        copy.start()
        return copy

    c_kx = send(0, k_ref, kx_ref, nx)
    c_vy = send(1, v_ref, vy_ref, ny)
    c_o = send(4, o_ref, o2_ref.at[core], nc)
    c_do = send(5, do_ref, do2_ref.at[core], nc)
    c_lse = send(6, lse_ref, lraw_ref.at[core], nc)
    c_q = send(7, q_ref, q2_ref.at[core], nc)
    c_vx = send(2, v_ref, vx_ref, nx)
    c_ky = send(3, k_ref, ky_ref, ny)

    loads = [pltpu.make_async_copy(s, r.at[core], load_sem.at[i])
             for i, (s, r) in enumerate([(do_ref, do2_ref), (o_ref, o2_ref), (lse_ref, lraw_ref), (q_ref, q2_ref)])]
    for load in loads:
        load.start()

    n_rows = ids_ref.shape[0]
    n_sub = lraw_ref.shape[1]
    pad = mark_ref.shape[0]
    load_ids = pltpu.make_async_copy(ids_ref, mark_ref.at[pl.ds(0, n_rows)], load_sem.at[4])
    load_ids.start()
    mark_ref[pl.ds(n_rows, pad - n_rows), :] = jnp.zeros((pad - n_rows, 128), jnp.int32)
    load_ids.wait()
    ids = mark_ref[...]
    lane = lax.broadcasted_iota(jnp.int32, (pad, 128), 1)
    row = lax.broadcasted_iota(jnp.int32, (pad, 128), 0)
    prev = pltpu.roll(ids, 1, axis=1)
    prev = jnp.where(lane == 0, pltpu.roll(prev, 1, axis=0), prev)
    acc = jnp.where(ids != prev, row * 128 + lane, 0)
    for sh in (1, 2, 4, 8, 16, 32, 64):
        acc = jnp.maximum(acc, jnp.where(lane >= sh, pltpu.roll(acc, sh, axis=1), 0))
    carry = jnp.max(acc, axis=1, keepdims=True) + jnp.zeros((pad, 128), jnp.int32)
    carry = jnp.where(row >= 1, pltpu.roll(carry, 1, axis=0), 0)
    sh = 1
    while sh < pad:
        carry = jnp.maximum(carry, jnp.where(row >= sh, pltpu.roll(carry, sh, axis=0), 0))
        sh *= 2
    starts = jnp.maximum(acc, carry).astype(jnp.float32)

    def hdot(a, b, dims=None):
        dims = (((1,), (0,)), ((), ())) if dims is None else dims
        return lax.dot_general(a, b, dims, precision=HIGHEST, preferred_element_type=jnp.float32)

    per = sub_len // 128
    off = (me // 2) * 2 * loc
    r_sub = lax.broadcasted_iota(jnp.int32, (n_sub, pad), 0)
    r_row = lax.broadcasted_iota(jnp.int32, (n_sub, pad), 1)
    pick = jnp.where(r_row == pre // 128 + per * r_sub + off // 128, 1.0, 0.0)
    sub_starts = hdot(pick, starts)
    src = lax.broadcasted_iota(jnp.int32, (128, 128), 0)
    dst = lax.broadcasted_iota(jnp.int32, (128, 128), 1)
    for e in range(2):
        spread = jnp.where(src == lax.rem(off, 128) + e * loc + dst // heads, 1.0, 0.0)
        rows_start = hdot(sub_starts, spread)
        start_ref[e] = rows_start.astype(jnp.int32)
        if e == 0:
            head = jnp.where(lax.broadcasted_iota(jnp.int32, (8, 128), 1) == 0, 1.0, 0.0)
            first_ref[...] = hdot(head, rows_start, NT).astype(jnp.int32)

    def delta_of(e, o_part):
        def body(t, c):
            r0 = pl.multiple_of(t * 128, 128)
            prod = do2_ref[e, pl.ds(r0, 128), :].astype(jnp.float32) * o_part[pl.ds(r0, 128), :].astype(jnp.float32)
            delta_ref[e, pl.ds(t, 1), :] = jnp.sum(prod.T, axis=0, keepdims=True)
            return c

        lax.fori_loop(0, n_sub, body, 0)

    for load in loads:
        load.wait()
    delta_of(core, o2_ref.at[core])
    c_o.wait_recv()
    c_do.wait_recv()
    delta_of(1 - core, o2_ref.at[1 - core])
    c_kx.wait_recv()
    c_kd = send(8, kx_ref, kd_ref, ny)
    c_vy.wait_recv()
    c_vd = send(9, vy_ref, vd_ref, nx)
    c_lse.wait_recv()
    tok = lax.broadcasted_iota(jnp.int32, (loc, 128), 0)
    tok_lane = lax.broadcasted_iota(jnp.int32, (loc, 128), 1)
    tok_spread = jnp.where(tok == tok_lane // heads, 1.0, 0.0)
    head_of = lax.broadcasted_iota(jnp.int32, (n_sub * heads, 128), 0)
    head_lane = lax.broadcasted_iota(jnp.int32, (n_sub * heads, 128), 1)
    own_head = lax.rem(head_of, heads) == lax.rem(head_lane, heads)
    g_sub = lax.broadcasted_iota(jnp.int32, (n_sub, n_sub * heads), 0)
    g_row = lax.broadcasted_iota(jnp.int32, (n_sub, n_sub * heads), 1)
    group = jnp.where(g_row // heads == g_sub, 1.0, 0.0)
    for e in range(2):
        wide = hdot(lraw_ref[e].reshape(n_sub * heads, loc), tok_spread)
        lse2_ref[e] = hdot(group, jnp.where(own_head, wide, 0.0)) * LOG2E
    c_q.wait_recv()
    c_vx.wait_recv()
    c_ky.wait_recv()
    c_kd.wait_recv()
    c_vd.wait_recv()
    for copy in (c_kx, c_vy, c_vx, c_ky, c_o, c_do, c_lse, c_q, c_kd, c_vd):
        copy.wait_send()


def split_kernel(dq_ref, own_ref, other_ref):
    n_sub, _, rows = dq_ref.shape
    half = rows // 2
    core = lax.rem(lax.axis_index('cp'), 2)
    mine = pl.multiple_of(core * half, half)
    theirs = pl.multiple_of((1 - core) * half, half)

    def put(t, c):
        r0 = pl.multiple_of(t * half, half)
        other_ref[pl.ds(r0, half), :] = dq_ref[t, :, pl.ds(theirs, half)].T
        own_ref[pl.ds(r0, half), :] = dq_ref[t, :, pl.ds(mine, half)].T
        return c

    lax.fori_loop(0, n_sub, put, 0)


def attn_kernel(*refs, owner_bits, has_dq, scale, pre, sub_len, loc, heads):
    n_in = 9 if has_dq else 8
    first_ref, q_ref, do_ref, lse_ref, delta_ref, start_ref, k_ref, v_ref = refs[:8]
    dq_ref, dk_ref, dv_ref, it_t, it_k, it_lo = refs[n_in:]
    me = lax.axis_index('cp')
    owner = me
    for bit in owner_bits:
        owner = flip(owner, bit)
    blk = k_ref.shape[0]
    n_sub, half = lse_ref.shape[1], lse_ref.shape[2]
    rows = 2 * half
    blo = owner * blk
    pos0 = pre + (me // 2) * 2 * loc
    dk_ref[...] = jnp.zeros_like(dk_ref)
    dv_ref[...] = jnp.zeros_like(dv_ref)
    if has_dq:
        dq_ref[...] = refs[8][...]
    else:
        dq_ref[...] = jnp.zeros_like(dq_ref)

    def more(c):
        return (c[0] < n_sub) & (first_ref[0, jnp.minimum(c[0], n_sub - 1)] < blo + blk)

    def add_tile(c):
        t, n = c
        lo = jnp.maximum(first_ref[0, t], blo)
        hi = jnp.minimum(pos0 + t * sub_len + 2 * loc - 1, blo + blk - 1)
        off = (lo - blo) // 16 * 16
        cnt = (hi - blo - off) // KT + 1

        def add_item(i, m):
            it_t[m] = t
            it_k[m] = jnp.minimum(off + i * KT, blk - KT)
            it_lo[m] = blo + off + i * KT
            return m + 1

        return t + 1, lax.fori_loop(0, cnt, add_item, n)

    t_first = jnp.maximum(blo - pos0 - 2 * loc + sub_len, 0) // sub_len
    n_items = lax.while_loop(more, add_tile, (t_first, 0))[1]
    for u in range(UNROLL - 1):
        it_t[n_items + u] = 0
        it_k[n_items + u] = 0
        it_lo[n_items + u] = 1 << 30

    def two(ref, t):
        return jnp.concatenate([ref[0, pl.ds(t, 1), :], ref[1, pl.ds(t, 1), :]], axis=1)

    lane = lax.broadcasted_iota(jnp.int32, (1, rows), 1)

    def body(w, c):
        st = []
        for u in range(UNROLL):
            m = w * UNROLL + u
            t = it_t[m]
            k0 = pl.multiple_of(it_k[m], 16)
            r0 = pl.multiple_of(t * half, half)
            k = k_ref[pl.ds(k0, KT), :]
            v = v_ref[pl.ds(k0, KT), :]
            q = jnp.concatenate([q_ref[0, pl.ds(r0, half), :], q_ref[1, pl.ds(r0, half), :]], axis=0)
            do = jnp.concatenate([do_ref[0, pl.ds(r0, half), :], do_ref[1, pl.ds(r0, half), :]], axis=0)
            s = lax.dot_general(k, q, NT, preferred_element_type=jnp.float32)
            dp = lax.dot_general(v, do, NT, preferred_element_type=jnp.float32)
            st.append((m, t, k0, k, q, do, s, dp))
        mid = []
        for u in range(UNROLL):
            m, t, k0, k, q, do, s, dp = st[u]
            lo = jnp.maximum(two(start_ref, t), it_lo[m])
            qpos = lane // heads + (pos0 + t * sub_len)
            kpos = lax.broadcasted_iota(jnp.int32, (KT, rows), 0) + (k0 + blo)
            allowed = (kpos >= lo) & (kpos <= qpos)
            p = jnp.where(allowed, jnp.exp2(s * (scale * LOG2E) - two(lse_ref, t)), 0.0)
            ds = (p * (dp - two(delta_ref, t))).astype(jnp.bfloat16)
            mid.append((p.astype(jnp.bfloat16), ds))
        for u in range(UNROLL):
            m, t, k0, k, q, do, s, dp = st[u]
            p, ds = mid[u]
            dv_ref[pl.ds(k0, KT), :] += jnp.dot(p, do, preferred_element_type=jnp.float32)
            dk_ref[pl.ds(k0, KT), :] += jnp.dot(ds, q, preferred_element_type=jnp.float32)
            dq_ref[t] += jnp.dot(k.T, ds, preferred_element_type=jnp.float32)
        return c

    lax.fori_loop(0, (n_items + UNROLL - 1) // UNROLL, body, 0)


def solution(mesh):
    cp = mesh.shape['cp']
    q_spec = P(None, 'cp', 'tp', None)
    lse_spec = P(None, 'cp', 'tp')
    kv_spec = P('cp', 'tp', None)

    def swap(x, bits):
        return lax.ppermute(x, 'cp', [(i, i ^ bits) for i in range(cp)])

    def local_backward(query, out_act, out_grad, row_lse, key_act, value_act, doc_ids):
        n_sub, loc, heads, d = query.shape
        blk = key_act.shape[0]
        n_keys = blk * cp
        half = loc * heads
        sub_len = loc * cp
        pre = n_keys - n_sub * sub_len
        scale = d ** -0.5
        f32, bf16, i32 = jnp.float32, jnp.bfloat16, jnp.int32
        dims = dict(pre=pre, sub_len=sub_len, loc=loc, heads=heads)
        vm = pl.BlockSpec(memory_space=VMEM)
        sm = pl.BlockSpec(memory_space=SMEM)
        hbm = pl.BlockSpec(memory_space=pltpu.HBM)
        sds = jax.ShapeDtypeStruct
        k_own, v_own = key_act.reshape(blk, d), value_act.reshape(blk, d)
        pad = (n_keys // 128 + 7) // 8 * 8
        kx, vx, ky, vy, kd, vd, q2, do2, lse2, delta, start, first = pl.pallas_call(
            functools.partial(gather_kernel, **dims),
            out_shape=tuple([sds((blk, d), bf16)] * 6 + [sds((2, n_sub * half, d), bf16)] * 2
                            + [sds((2, n_sub, half), f32)] * 2 + [sds((2, n_sub, half), i32), sds((8, n_sub), i32)]),
            in_specs=[hbm] * 7, out_specs=(vm,) * 12,
            scratch_shapes=[VMEM((2, n_sub * half, d), bf16), VMEM((2, n_sub, heads, loc), f32), VMEM((pad, 128), i32),
                            pltpu.SemaphoreType.DMA((10,)), pltpu.SemaphoreType.DMA((10,)), pltpu.SemaphoreType.DMA((5,))],
            compiler_params=pltpu.CompilerParams(collective_id=0, has_side_effects=True, vmem_limit_bytes=24 * 2 ** 20),
            name='gather_kv',
        )(*[pltpu.with_memory_space_constraint(x, pltpu.HBM) for x in (
            k_own, v_own, query.reshape(-1, d), out_grad.reshape(-1, d), out_act.reshape(-1, d),
            row_lse.transpose(0, 2, 1), doc_ids.reshape(n_keys // 128, 128))])

        cap = n_sub * (-(-blk // KT) + 1) + UNROLL
        items = [SMEM((cap,), i32)] * 3
        acc = sds((n_sub, d, 2 * half), f32)
        kv_out = sds((blk, d), f32)
        dq_out = sds((n_sub * half, d), f32)
        cost = pl.CostEstimate(flops=2 * 10 ** 9, bytes_accessed=10 ** 7, transcendentals=10 ** 6)

        def attend(bits, k, v, dq=None):
            ins = [first, q2, do2, lse2, delta, start, k, v] + ([dq] if dq is not None else [])
            return pl.pallas_call(
                functools.partial(attn_kernel, owner_bits=bits, has_dq=dq is not None, scale=scale, **dims),
                out_shape=(acc, kv_out, kv_out), in_specs=[sm] + [vm] * (len(ins) - 1), out_specs=(vm,) * 3,
                scratch_shapes=items,
                compiler_params=pltpu.CompilerParams(vmem_limit_bytes=28 * 2 ** 20),
                cost_estimate=cost, name='attn_bwd')(*ins)

        def run(bits, k, v, dq=None):
            return attend(bits, k, v, dq)

        dq, dk_d, dv_d = run((2, 4), kd, vd)
        got_ky = swap(dk_d, 2)
        got_vx = swap(dv_d, 4)
        dq, dk_x, dv_x = run((2,), kx, vx, dq)
        got_ko = swap(dk_x, 2)
        dq, dk_y, dv_y = run((4,), ky, vy, dq)
        got_vo = swap(dv_y, 4)
        last_k = swap(dk_y + got_ky, 4)
        last_v = swap(dv_x + got_vx, 2)
        dq, dk_o, dv_o = run((), k_own, v_own, dq)
        dq_own, dq_other = pl.pallas_call(
            split_kernel, out_shape=(dq_out, dq_out), in_specs=[vm], out_specs=(vm, vm),
            compiler_params=pltpu.CompilerParams(vmem_limit_bytes=28 * 2 ** 20), name='split_dq')(dq)
        got_dq = swap(dq_other, 1)
        d_query = ((dq_own + got_dq) * scale).astype(bf16)
        d_key = (dk_o + got_ko + last_k) * scale
        d_value = dv_o + got_vo + last_v
        return d_query.reshape(query.shape), d_key.reshape(key_act.shape), d_value.reshape(value_act.shape)

    return jax.shard_map(local_backward, mesh=mesh, in_specs=(q_spec, q_spec, q_spec, lse_spec, kv_spec, kv_spec, P()), out_specs=(q_spec, kv_spec, kv_spec), check_vma=False)
```

```python
import functools

import jax
import jax.numpy as jnp
from jax import lax
from jax.experimental import pallas as pl
from jax.experimental.pallas import tpu as pltpu
from jax.sharding import PartitionSpec as P


LOG2E = 1.4426950408889634
NT = (((1,), (1,)), ((), ()))
MESH = pl.DeviceIdType.MESH
VMEM, SMEM = pltpu.VMEM, pltpu.SMEM
HIGHEST = lax.Precision.HIGHEST
KT = 256
UNROLL = 4


def flip(me, bit):
    return me + bit - 2 * bit * lax.rem(me // bit, 2)


def prep_kernel(k_ref, v_ref, q_ref, do_ref, o_ref, lse_ref, ids_ref,
                kx_ref, vx_ref, ky_ref, vy_ref, q2_ref, do2_ref, lse2_ref, delta_ref, start_ref, first_ref,
                o2_ref, lraw_ref, mark_ref, send_sem, recv_sem, load_sem, *, pre, sub_len, loc, heads):
    me = lax.axis_index('cp')
    core = lax.rem(me, 2)
    nx, ny, partner = flip(me, 2), flip(me, 4), flip(me, 1)
    barrier = pltpu.get_barrier_semaphore()
    for other in (nx, ny, partner):
        pl.semaphore_signal(barrier, inc=1, device_id={'cp': other}, device_id_type=MESH)
    pl.semaphore_wait(barrier, 3)
    pairs = [(do_ref, do2_ref), (o_ref, o2_ref), (lse_ref, lraw_ref), (q_ref, q2_ref)]
    moves = [(s, r.at[core], partner) for s, r in pairs]
    moves += [(k_ref, kx_ref, nx), (v_ref, vy_ref, ny), (v_ref, vx_ref, nx), (k_ref, ky_ref, ny)]
    sends = [pltpu.make_async_remote_copy(src_ref=s, dst_ref=r, send_sem=send_sem.at[i], recv_sem=recv_sem.at[i],
                                          device_id={'cp': to}, device_id_type=MESH) for i, (s, r, to) in enumerate(moves)]
    loads = [pltpu.make_async_copy(s, r.at[core], load_sem.at[i]) for i, (s, r) in enumerate(pairs)]
    for copy in sends[4:] + sends[:4] + loads:
        copy.start()

    n_rows = ids_ref.shape[0]
    n_sub = lraw_ref.shape[1]
    pad = mark_ref.shape[0]
    load_ids = pltpu.make_async_copy(ids_ref, mark_ref.at[pl.ds(0, n_rows)], load_sem.at[4])
    load_ids.start()
    mark_ref[pl.ds(n_rows, pad - n_rows), :] = jnp.zeros((pad - n_rows, 128), jnp.int32)
    load_ids.wait()
    ids = mark_ref[...]
    lane = lax.broadcasted_iota(jnp.int32, (pad, 128), 1)
    row = lax.broadcasted_iota(jnp.int32, (pad, 128), 0)
    prev = pltpu.roll(ids, 1, axis=1)
    prev = jnp.where(lane == 0, pltpu.roll(prev, 1, axis=0), prev)
    acc = jnp.where(ids != prev, row * 128 + lane, 0)
    for sh in (1, 2, 4, 8, 16, 32, 64):
        acc = jnp.maximum(acc, jnp.where(lane >= sh, pltpu.roll(acc, sh, axis=1), 0))
    carry = jnp.max(acc, axis=1, keepdims=True) + jnp.zeros((pad, 128), jnp.int32)
    carry = jnp.where(row >= 1, pltpu.roll(carry, 1, axis=0), 0)
    sh = 1
    while sh < pad:
        carry = jnp.maximum(carry, jnp.where(row >= sh, pltpu.roll(carry, sh, axis=0), 0))
        sh *= 2
    starts = jnp.maximum(acc, carry).astype(jnp.float32)

    def hdot(a, b, dims=None):
        dims = (((1,), (0,)), ((), ())) if dims is None else dims
        return lax.dot_general(a, b, dims, precision=HIGHEST, preferred_element_type=jnp.float32)

    per = sub_len // 128
    off = (me // 2) * 2 * loc
    r_sub = lax.broadcasted_iota(jnp.int32, (n_sub, pad), 0)
    r_row = lax.broadcasted_iota(jnp.int32, (n_sub, pad), 1)
    pick = jnp.where(r_row == pre // 128 + per * r_sub + off // 128, 1.0, 0.0)
    sub_starts = hdot(pick, starts)
    src = lax.broadcasted_iota(jnp.int32, (128, 128), 0)
    dst = lax.broadcasted_iota(jnp.int32, (128, 128), 1)
    for e in range(2):
        spread = jnp.where(src == lax.rem(off, 128) + e * loc + dst // heads, 1.0, 0.0)
        rows_start = hdot(sub_starts, spread)
        start_ref[e] = rows_start.astype(jnp.int32)
        if e == 0:
            head = jnp.where(lax.broadcasted_iota(jnp.int32, (8, 128), 1) == 0, 1.0, 0.0)
            first_ref[...] = hdot(head, rows_start, NT).astype(jnp.int32)

    def delta_of(e, o_part):
        def body(t, c):
            r0 = pl.multiple_of(t * 128, 128)
            prod = do2_ref[e, pl.ds(r0, 128), :].astype(jnp.float32) * o_part[pl.ds(r0, 128), :].astype(jnp.float32)
            delta_ref[e, pl.ds(t, 1), :] = jnp.sum(prod.T, axis=0, keepdims=True)
            return c

        lax.fori_loop(0, n_sub, body, 0)

    for load in loads:
        load.wait()
    delta_of(core, o2_ref.at[core])
    for copy in sends[:3]:
        copy.wait_recv()
    delta_of(1 - core, o2_ref.at[1 - core])
    tok = lax.broadcasted_iota(jnp.int32, (loc, 128), 0)
    tok_lane = lax.broadcasted_iota(jnp.int32, (loc, 128), 1)
    tok_spread = jnp.where(tok == tok_lane // heads, 1.0, 0.0)
    head_of = lax.broadcasted_iota(jnp.int32, (n_sub * heads, 128), 0)
    head_lane = lax.broadcasted_iota(jnp.int32, (n_sub * heads, 128), 1)
    own_head = lax.rem(head_of, heads) == lax.rem(head_lane, heads)
    g_sub = lax.broadcasted_iota(jnp.int32, (n_sub, n_sub * heads), 0)
    g_row = lax.broadcasted_iota(jnp.int32, (n_sub, n_sub * heads), 1)
    group = jnp.where(g_row // heads == g_sub, 1.0, 0.0)
    for e in range(2):
        wide = hdot(lraw_ref[e].reshape(n_sub * heads, loc), tok_spread)
        lse2_ref[e] = hdot(group, jnp.where(own_head, wide, 0.0)) * LOG2E
    for copy in sends[3:]:
        copy.wait_recv()
    for copy in sends:
        copy.wait_send()


def split_kernel(dq_ref, own_ref, other_ref):
    n_sub, _, rows = dq_ref.shape
    half = rows // 2
    core = lax.rem(lax.axis_index('cp'), 2)
    mine = pl.multiple_of(core * half, half)
    theirs = pl.multiple_of((1 - core) * half, half)

    def put(t, c):
        r0 = pl.multiple_of(t * half, half)
        other_ref[pl.ds(r0, half), :] = dq_ref[t, :, pl.ds(theirs, half)].T
        own_ref[pl.ds(r0, half), :] = dq_ref[t, :, pl.ds(mine, half)].T
        return c

    lax.fori_loop(0, n_sub, put, 0)


def attn_kernel(*refs, blocks, row0, n_keys, outs, has_dq, scale, blk, pre, sub_len, loc, heads):
    first_ref, q_ref, do_ref, lse_ref, delta_ref, start_ref = refs[:6]
    nb = len(blocks)
    k_in, v_in, refs = refs[6:6 + nb], refs[6 + nb:6 + 2 * nb], refs[6 + 2 * nb:]
    if has_dq:
        dq_in, refs = refs[0], refs[1:]
    dq_ref, grad_out, refs = refs[0], refs[1:1 + len(outs)], refs[1 + len(outs):]
    it_t, it_k, it_lo, it_base, p_ref, ds_ref, kpos_ref, k_ref, v_ref, dk_ref, dv_ref = refs
    me = lax.axis_index('cp')
    n_sub, half = lse_ref.shape[1], lse_ref.shape[2]
    rows = 2 * half
    pos0 = pre + (me // 2) * 2 * loc
    for b in range(nb):
        k_ref[b * n_keys:(b + 1) * n_keys, :] = k_in[b][row0:row0 + n_keys, :]
        v_ref[b * n_keys:(b + 1) * n_keys, :] = v_in[b][row0:row0 + n_keys, :]
    dk_ref[...] = jnp.zeros_like(dk_ref)
    dv_ref[...] = jnp.zeros_like(dv_ref)
    if has_dq:
        dq_ref[...] = dq_in[...]
    else:
        dq_ref[...] = jnp.zeros_like(dq_ref)

    n_items = 0
    for b, bits in enumerate(blocks):
        owner = me
        for bit in bits:
            owner = flip(owner, bit)
        blo = owner * blk + row0

        def more(c, blo=blo):
            return (c[0] < n_sub) & (first_ref[0, jnp.minimum(c[0], n_sub - 1)] < blo + n_keys)

        def add_tile(c, b=b, blo=blo):
            t, n = c
            lo = jnp.maximum(first_ref[0, t], blo)
            hi = jnp.minimum(pos0 + t * sub_len + 2 * loc - 1, blo + n_keys - 1)
            off = (lo - blo) // 16 * 16
            cnt = (hi - blo - off) // KT + 1

            def add_item(i, m):
                it_t[m] = t
                it_k[m] = b * n_keys + jnp.minimum(off + i * KT, n_keys - KT)
                it_lo[m] = blo + off + i * KT
                it_base[m] = blo - b * n_keys
                return m + 1

            return t + 1, lax.fori_loop(0, cnt, add_item, n)

        t_first = jnp.maximum(blo - pos0 - 2 * loc + sub_len, 0) // sub_len
        n_items = lax.while_loop(more, add_tile, (t_first, n_items))[1]
    for u in range(UNROLL - 1):
        it_t[n_items + u] = 0
        it_k[n_items + u] = 0
        it_lo[n_items + u] = 1 << 30
        it_base[n_items + u] = 0

    def two(ref, t):
        return jnp.concatenate([ref[0, pl.ds(t, 1), :], ref[1, pl.ds(t, 1), :]], axis=1)

    lane = lax.broadcasted_iota(jnp.int32, (1, rows), 1)
    zero = jnp.zeros((16, rows), jnp.bfloat16)
    kpos_ref[...] = lax.broadcasted_iota(jnp.int32, (KT, rows), 0).astype(jnp.float32).astype(jnp.bfloat16)

    def item(w, u):
        m = w * UNROLL + u
        t = it_t[m]
        k0 = pl.multiple_of(it_k[m], 16)
        r0 = pl.multiple_of(t * half, half)
        q = jnp.concatenate([q_ref[0, pl.ds(r0, half), :], q_ref[1, pl.ds(r0, half), :]], axis=0)
        do = jnp.concatenate([do_ref[0, pl.ds(r0, half), :], do_ref[1, pl.ds(r0, half), :]], axis=0)
        return m, t, k0, q, do

    def scores(w):
        out = []
        for u in range(UNROLL):
            m, t, k0, q, do = item(w, u)
            s = lax.dot_general(k_ref[pl.ds(k0, KT), :], q, NT, preferred_element_type=jnp.float32)
            dp = lax.dot_general(v_ref[pl.ds(k0, KT), :], do, NT, preferred_element_type=jnp.float32)
            lo = jnp.maximum(two(start_ref, t), it_lo[m]) - (k0 + it_base[m])
            qpos = lane // heads + (pos0 + t * sub_len - k0 - it_base[m])
            lo = packed(jnp.clip(lo, 0, KT))
            qpos = packed(jnp.clip(qpos, -1, KT))
            out.append((s, dp, lo, qpos, two(lse_ref, t), two(delta_ref, t)))
        return out

    def packed(x):
        return jnp.broadcast_to(x.astype(jnp.float32), (16, rows)).astype(jnp.bfloat16)

    def probs(parts):
        for u in range(UNROLL):
            s, dp, lo, qpos, lse, delta = parts[u]
            for g in range(KT // 16):
                r = slice(16 * g, 16 * g + 16)
                kpos = kpos_ref[r, :]
                allowed = (kpos >= lo) & (kpos <= qpos)
                p = jnp.exp2(s[r, :] * (scale * LOG2E) - lse)
                ds = p * (dp[r, :] - delta)
                p_ref[u, r, :] = jnp.where(allowed, p.astype(jnp.bfloat16), zero)
                ds_ref[u, r, :] = jnp.where(allowed, ds.astype(jnp.bfloat16), zero)

    def grads(w):
        for u in range(UNROLL):
            _, t, k0, q, do = item(w, u)
            p, ds = p_ref[u], ds_ref[u]
            dv_ref[pl.ds(k0, KT), :] += jnp.dot(p, do, preferred_element_type=jnp.float32)
            dk_ref[pl.ds(k0, KT), :] += jnp.dot(ds, q, preferred_element_type=jnp.float32)
            dq_ref[t] += jnp.dot(k_ref[pl.ds(k0, KT), :].T, ds, preferred_element_type=jnp.float32)

    def body(w, c):
        probs(scores(w))
        grads(w)
        return c

    lax.fori_loop(0, (n_items + UNROLL - 1) // UNROLL, body, 0)
    for ref, (kind, which) in zip(grad_out, outs):
        acc = dk_ref if kind == 'k' else dv_ref
        ref[...] = acc[which[0] * n_keys:(which[-1] + 1) * n_keys, :]


def solution(mesh):
    cp = mesh.shape['cp']
    q_spec = P(None, 'cp', 'tp', None)
    lse_spec = P(None, 'cp', 'tp')
    kv_spec = P('cp', 'tp', None)

    def swap(x, bits):
        return lax.ppermute(x, 'cp', [(i, i ^ bits) for i in range(cp)])

    def local_backward(query, out_act, out_grad, row_lse, key_act, value_act, doc_ids):
        n_sub, loc, heads, d = query.shape
        blk = key_act.shape[0]
        n_keys = blk * cp
        half = loc * heads
        sub_len = loc * cp
        pre = n_keys - n_sub * sub_len
        scale = d ** -0.5
        f32, bf16, i32 = jnp.float32, jnp.bfloat16, jnp.int32
        dims = dict(pre=pre, sub_len=sub_len, loc=loc, heads=heads)
        vm = pl.BlockSpec(memory_space=VMEM)
        sm = pl.BlockSpec(memory_space=SMEM)
        hbm = pl.BlockSpec(memory_space=pltpu.HBM)
        sds = jax.ShapeDtypeStruct
        k_own, v_own = key_act.reshape(blk, d), value_act.reshape(blk, d)
        pad = (n_keys // 128 + 7) // 8 * 8
        acc = sds((n_sub, d, 2 * half), f32)
        dq_out = sds((n_sub * half, d), f32)
        cost = pl.CostEstimate(flops=2 * 10 ** 9, bytes_accessed=10 ** 7, transcendentals=10 ** 6)

        def attend(keys, values, dq, blocks, row0, n_rows, outs):
            nb = len(blocks)
            ins = [first, q2, do2, lse2, delta, start, *keys, *values] + ([dq] if dq is not None else [])
            cap = nb * n_sub * (-(-n_rows // KT) + 1) + UNROLL
            kv = (nb * n_rows, d)
            return pl.pallas_call(
                functools.partial(attn_kernel, blocks=blocks, row0=row0, n_keys=n_rows, outs=outs, has_dq=dq is not None,
                                  scale=scale, blk=blk, **dims),
                out_shape=(acc,) + tuple(sds((len(w) * n_rows, d), f32) for _, w in outs),
                in_specs=[sm] + [vm] * (len(ins) - 1), out_specs=(vm,) * (1 + len(outs)),
                scratch_shapes=[SMEM((cap,), i32)] * 4 + [VMEM((UNROLL, KT, 2 * half), bf16)] * 2 + [VMEM((KT, 2 * half), bf16)]
                + [VMEM(kv, bf16)] * 2 + [VMEM(kv, f32)] * 2,
                compiler_params=pltpu.CompilerParams(vmem_limit_bytes=28 * 2 ** 20),
                cost_estimate=cost, name='attn_bwd')(*ins)

        kx, vx, ky, vy, q2, do2, lse2, delta, start, first = pl.pallas_call(
            functools.partial(prep_kernel, **dims),
            out_shape=tuple([sds((blk, d), bf16)] * 4 + [sds((2, n_sub * half, d), bf16)] * 2 + [sds((2, n_sub, half), f32)] * 2
                            + [sds((2, n_sub, half), i32), sds((8, n_sub), i32)]),
            in_specs=[hbm] * 7, out_specs=(vm,) * 10,
            scratch_shapes=[VMEM((2, n_sub * half, d), bf16), VMEM((2, n_sub, heads, loc), f32), VMEM((pad, 128), i32),
                            pltpu.SemaphoreType.DMA((8,)), pltpu.SemaphoreType.DMA((8,)), pltpu.SemaphoreType.DMA((5,))],
            compiler_params=pltpu.CompilerParams(collective_id=0, has_side_effects=True, vmem_limit_bytes=24 * 2 ** 20),
            name='prep',
        )(*[pltpu.with_memory_space_constraint(x, pltpu.HBM) for x in (
            k_own, v_own, query.reshape(-1, d), out_grad.reshape(-1, d), out_act.reshape(-1, d),
            row_lse.transpose(0, 2, 1), doc_ids.reshape(n_keys // 128, 128))])
        kd = swap(kx, 4)
        vd = swap(vy, 2)
        both = (('k', (0,)), ('v', (0,)))
        four = (('k', (0,)), ('k', (1,)), ('v', (0,)), ('v', (1,)))
        dq, dk_x, dk_y, dv_x, dv_y = attend([kx, ky], [vx, vy], None, ((2,), (4,)), 0, blk, four)
        got_ko = swap(dk_x, 2)
        got_vo = swap(dv_y, 4)
        dq, dk_d, dv_d = attend([kd], [vd], dq, ((2, 4),), 0, blk, both)
        got_ky = swap(dk_d, 2)
        got_vx = swap(dv_d, 4)
        dq, dk_o, dv_o = attend([k_own], [v_own], dq, ((),), 0, blk, both)
        last_k = swap(dk_y + got_ky, 4)
        last_v = swap(dv_x + got_vx, 2)
        dq_own, dq_other = pl.pallas_call(
            split_kernel, out_shape=(dq_out, dq_out), in_specs=[vm], out_specs=(vm, vm),
            compiler_params=pltpu.CompilerParams(vmem_limit_bytes=28 * 2 ** 20), name='split_dq')(dq)
        got_dq = swap(dq_other, 1)
        d_query = ((dq_own + got_dq) * scale).astype(bf16)
        d_key = (dk_o + got_ko + last_k) * scale
        d_value = dv_o + got_vo + last_v
        return d_query.reshape(query.shape), d_key.reshape(key_act.shape), d_value.reshape(value_act.shape)

    return jax.shard_map(local_backward, mesh=mesh, in_specs=(q_spec, q_spec, q_spec, lse_spec, kv_spec, kv_spec, P()), out_specs=(q_spec, kv_spec, kv_spec), check_vma=False)
```

```python
import functools

import jax
import jax.numpy as jnp
from jax import lax
from jax.experimental import pallas as pl
from jax.experimental.pallas import tpu as pltpu
from jax.sharding import PartitionSpec as P


LOG2E = 1.4426950408889634
NT = (((1,), (1,)), ((), ()))
MESH = pl.DeviceIdType.MESH
VMEM, SMEM = pltpu.VMEM, pltpu.SMEM
HIGHEST = lax.Precision.HIGHEST
KT = 256
SMALL = 128
MAIN, MAIN_SMALL, TAIL = 6, 6, 2


def flip(me, bit):
    return me + bit - 2 * bit * lax.rem(me // bit, 2)


def prep_kernel(k_ref, v_ref, q_ref, do_ref, o_ref, lse_ref, ids_ref,
                kx_ref, vx_ref, ky_ref, vy_ref, q2_ref, do2_ref, lse2_ref, delta_ref, start_ref, first_ref,
                o2_ref, lraw_ref, mark_ref, send_sem, recv_sem, load_sem, *, pre, sub_len, loc, heads):
    me = lax.axis_index('cp')
    core = lax.rem(me, 2)
    nx, ny, partner = flip(me, 2), flip(me, 4), flip(me, 1)
    barrier = pltpu.get_barrier_semaphore()
    for other in (nx, ny, partner):
        pl.semaphore_signal(barrier, inc=1, device_id={'cp': other}, device_id_type=MESH)
    pl.semaphore_wait(barrier, 3)
    pairs = [(do_ref, do2_ref), (o_ref, o2_ref), (lse_ref, lraw_ref), (q_ref, q2_ref)]
    moves = [(s, r.at[core], partner) for s, r in pairs]
    moves += [(k_ref, kx_ref, nx), (v_ref, vy_ref, ny), (v_ref, vx_ref, nx), (k_ref, ky_ref, ny)]
    sends = [pltpu.make_async_remote_copy(src_ref=s, dst_ref=r, send_sem=send_sem.at[i], recv_sem=recv_sem.at[i],
                                          device_id={'cp': to}, device_id_type=MESH) for i, (s, r, to) in enumerate(moves)]
    loads = [pltpu.make_async_copy(s, r.at[core], load_sem.at[i]) for i, (s, r) in enumerate(pairs)]
    for copy in sends[4:] + sends[:4] + loads:
        copy.start()

    n_rows = ids_ref.shape[0]
    n_sub = lraw_ref.shape[1]
    pad = mark_ref.shape[0]
    load_ids = pltpu.make_async_copy(ids_ref, mark_ref.at[pl.ds(0, n_rows)], load_sem.at[4])
    load_ids.start()
    mark_ref[pl.ds(n_rows, pad - n_rows), :] = jnp.zeros((pad - n_rows, 128), jnp.int32)
    load_ids.wait()
    ids = mark_ref[...]
    lane = lax.broadcasted_iota(jnp.int32, (pad, 128), 1)
    row = lax.broadcasted_iota(jnp.int32, (pad, 128), 0)
    prev = pltpu.roll(ids, 1, axis=1)
    prev = jnp.where(lane == 0, pltpu.roll(prev, 1, axis=0), prev)
    acc = jnp.where(ids != prev, row * 128 + lane, 0)
    for sh in (1, 2, 4, 8, 16, 32, 64):
        acc = jnp.maximum(acc, jnp.where(lane >= sh, pltpu.roll(acc, sh, axis=1), 0))
    carry = jnp.max(acc, axis=1, keepdims=True) + jnp.zeros((pad, 128), jnp.int32)
    carry = jnp.where(row >= 1, pltpu.roll(carry, 1, axis=0), 0)
    sh = 1
    while sh < pad:
        carry = jnp.maximum(carry, jnp.where(row >= sh, pltpu.roll(carry, sh, axis=0), 0))
        sh *= 2
    starts = jnp.maximum(acc, carry).astype(jnp.float32)

    def hdot(a, b, dims=None):
        dims = (((1,), (0,)), ((), ())) if dims is None else dims
        return lax.dot_general(a, b, dims, precision=HIGHEST, preferred_element_type=jnp.float32)

    per = sub_len // 128
    off = (me // 2) * 2 * loc
    r_sub = lax.broadcasted_iota(jnp.int32, (n_sub, pad), 0)
    r_row = lax.broadcasted_iota(jnp.int32, (n_sub, pad), 1)
    pick = jnp.where(r_row == pre // 128 + per * r_sub + off // 128, 1.0, 0.0)
    sub_starts = hdot(pick, starts)
    src = lax.broadcasted_iota(jnp.int32, (128, 128), 0)
    dst = lax.broadcasted_iota(jnp.int32, (128, 128), 1)
    for e in range(2):
        spread = jnp.where(src == lax.rem(off, 128) + e * loc + dst // heads, 1.0, 0.0)
        rows_start = hdot(sub_starts, spread)
        start_ref[e] = rows_start.astype(jnp.int32)
        if e == 0:
            head = jnp.where(lax.broadcasted_iota(jnp.int32, (8, 128), 1) == 0, 1.0, 0.0)
            first_ref[...] = hdot(head, rows_start, NT).astype(jnp.int32)

    def delta_of(e, o_part):
        def body(t, c):
            r0 = pl.multiple_of(t * 128, 128)
            prod = do2_ref[e, pl.ds(r0, 128), :].astype(jnp.float32) * o_part[pl.ds(r0, 128), :].astype(jnp.float32)
            delta_ref[e, pl.ds(t, 1), :] = jnp.sum(prod.T, axis=0, keepdims=True)
            return c

        lax.fori_loop(0, n_sub, body, 0)

    for load in loads:
        load.wait()
    delta_of(core, o2_ref.at[core])
    for copy in sends[:3]:
        copy.wait_recv()
    delta_of(1 - core, o2_ref.at[1 - core])
    tok = lax.broadcasted_iota(jnp.int32, (loc, 128), 0)
    tok_lane = lax.broadcasted_iota(jnp.int32, (loc, 128), 1)
    tok_spread = jnp.where(tok == tok_lane // heads, 1.0, 0.0)
    head_of = lax.broadcasted_iota(jnp.int32, (n_sub * heads, 128), 0)
    head_lane = lax.broadcasted_iota(jnp.int32, (n_sub * heads, 128), 1)
    own_head = lax.rem(head_of, heads) == lax.rem(head_lane, heads)
    g_sub = lax.broadcasted_iota(jnp.int32, (n_sub, n_sub * heads), 0)
    g_row = lax.broadcasted_iota(jnp.int32, (n_sub, n_sub * heads), 1)
    group = jnp.where(g_row // heads == g_sub, 1.0, 0.0)
    for e in range(2):
        wide = hdot(lraw_ref[e].reshape(n_sub * heads, loc), tok_spread)
        lse2_ref[e] = hdot(group, jnp.where(own_head, wide, 0.0)) * LOG2E
    for copy in sends[3:]:
        copy.wait_recv()
    for copy in sends:
        copy.wait_send()


def finish_kernel(own_ref, got_ref, out_ref, *, scale):
    half = own_ref.shape[2]

    step = 4

    def put(i, c):
        for u in range(step):
            t = i * step + u
            total = (own_ref[t] + got_ref[t]) * scale
            out_ref[pl.ds(pl.multiple_of(t * half, half), half), :] = total.T.astype(jnp.bfloat16)
        return c

    lax.fori_loop(0, own_ref.shape[0] // step, put, 0)


def attn_kernel(*refs, blocks, n_keys, outs, has_dq, last, scale, blk, pre, sub_len, loc, heads):
    first_ref, q_ref, do_ref, lse_ref, delta_ref, start_ref = refs[:6]
    nb = len(blocks)
    k_in, v_in, refs = refs[6:6 + nb], refs[6 + nb:6 + 2 * nb], refs[6 + 2 * nb:]
    if has_dq:
        dq_in, refs = refs[0], refs[1:]
    n_dq = 2 if last else 1
    dq_out, grad_out, refs = refs[:n_dq], refs[n_dq:n_dq + len(outs)], refs[n_dq + len(outs):]
    it_t, it_k, it_lo, it_base, p_ref, ds_ref, kpos_ref, refs = *refs[:7], refs[7:]
    if last:
        dq_ref, refs = refs[0], refs[1:]
    else:
        dq_ref = dq_out[0]
    if nb == 1:
        k_ref, v_ref, dk_ref, dv_ref = k_in[0], v_in[0], grad_out[0], grad_out[1]
    else:
        k_ref, v_ref, dk_ref, dv_ref = refs
    me = lax.axis_index('cp')
    n_sub, half = lse_ref.shape[1], lse_ref.shape[2]
    rows = 2 * half
    pos0 = pre + (me // 2) * 2 * loc
    if nb > 1:
        for b in range(nb):
            k_ref[b * n_keys:(b + 1) * n_keys, :] = k_in[b][...]
            v_ref[b * n_keys:(b + 1) * n_keys, :] = v_in[b][...]
    dk_ref[...] = jnp.zeros_like(dk_ref)
    dv_ref[...] = jnp.zeros_like(dv_ref)
    if has_dq:
        dq_ref[...] = dq_in[...]
    else:
        dq_ref[...] = jnp.zeros_like(dq_ref)

    cap = it_t.shape[0] // 2

    def put_item(m, t, b, row, lo, blo, kt):
        it_t[m] = t
        it_k[m] = b * n_keys + jnp.minimum(row, n_keys - kt)
        it_lo[m] = lo
        it_base[m] = blo - b * n_keys

    n_items, n_small = 0, 0
    for b, bits in enumerate(blocks):
        owner = me
        for bit in bits:
            owner = flip(owner, bit)
        blo = owner * blk

        def more(c, blo=blo):
            return (c[0] < n_sub) & (first_ref[0, jnp.minimum(c[0], n_sub - 1)] < blo + n_keys)

        def add_tile(c, b=b, blo=blo):
            t, n, ns = c
            lo = jnp.maximum(first_ref[0, t], blo)
            hi = jnp.minimum(pos0 + t * sub_len + 2 * loc - 1, blo + n_keys - 1)
            off = (lo - blo) // 16 * 16
            length = hi - blo - off + 1
            full = length // KT
            rest = length - full * KT
            cnt = full + jnp.where(rest > SMALL, 1, 0)

            def add_item(i, m):
                put_item(m, t, b, off + i * KT, blo + off + i * KT, blo, KT)
                return m + 1

            put_item(cap + ns, t, b, off + full * KT, blo + off + full * KT, blo, SMALL)
            ns = ns + jnp.where((rest > 0) & (rest <= SMALL), 1, 0)
            return t + 1, lax.fori_loop(0, cnt, add_item, n), ns

        t_first = jnp.maximum(blo - pos0 - 2 * loc + sub_len, 0) // sub_len
        _, n_items, n_small = lax.while_loop(more, add_tile, (t_first, n_items, n_small))
    for n in (n_items, cap + n_small):
        put_item(n, 0, 0, 0, 1 << 30, 0, KT)

    def two(ref, t):
        return jnp.concatenate([ref[0, pl.ds(t, 1), :], ref[1, pl.ds(t, 1), :]], axis=1)

    lane = lax.broadcasted_iota(jnp.int32, (1, rows), 1)
    zero = jnp.zeros((16, rows), jnp.bfloat16)
    kpos_ref[...] = lax.broadcasted_iota(jnp.int32, (KT, rows), 0).astype(jnp.float32).astype(jnp.bfloat16)

    def item(m):
        t = it_t[m]
        k0 = pl.multiple_of(it_k[m], 16)
        r0 = pl.multiple_of(t * half, half)
        q = jnp.concatenate([q_ref[0, pl.ds(r0, half), :], q_ref[1, pl.ds(r0, half), :]], axis=0)
        do = jnp.concatenate([do_ref[0, pl.ds(r0, half), :], do_ref[1, pl.ds(r0, half), :]], axis=0)
        return t, k0, q, do

    def scores(first, n, kt):
        out = []
        for u in range(n):
            m = first + u
            t, k0, q, do = item(m)
            s = lax.dot_general(k_ref[pl.ds(k0, kt), :], q, NT, preferred_element_type=jnp.float32)
            dp = lax.dot_general(v_ref[pl.ds(k0, kt), :], do, NT, preferred_element_type=jnp.float32)
            lo = jnp.maximum(two(start_ref, t), it_lo[m]) - (k0 + it_base[m])
            qpos = lane // heads + (pos0 + t * sub_len - k0 - it_base[m])
            lo = packed(jnp.clip(lo, 0, KT))
            qpos = packed(jnp.clip(qpos, -1, KT))
            out.append((s, dp, lo, qpos, two(lse_ref, t), two(delta_ref, t)))
        return out

    def packed(x):
        return jnp.broadcast_to(x.astype(jnp.float32), (16, rows)).astype(jnp.bfloat16)

    def probs(parts, kt):
        for u in range(len(parts)):
            s, dp, lo, qpos, lse, delta = parts[u]
            for g in range(kt // 16):
                r = slice(16 * g, 16 * g + 16)
                kpos = kpos_ref[r, :]
                allowed = (kpos >= lo) & (kpos <= qpos)
                p = jnp.exp2(s[r, :] * (scale * LOG2E) - lse)
                ds = p * (dp[r, :] - delta)
                p_ref[u, r, :] = jnp.where(allowed, p.astype(jnp.bfloat16), zero)
                ds_ref[u, r, :] = jnp.where(allowed, ds.astype(jnp.bfloat16), zero)

    def grads(first, n, kt):
        for u in range(n):
            t, k0, q, do = item(first + u)
            p, ds = p_ref[u, :kt, :], ds_ref[u, :kt, :]
            dv_ref[pl.ds(k0, kt), :] += jnp.dot(p, do, preferred_element_type=jnp.float32)
            dk_ref[pl.ds(k0, kt), :] += jnp.dot(ds, q, preferred_element_type=jnp.float32)
            dq_ref[t] += jnp.dot(k_ref[pl.ds(k0, kt), :].T, ds, preferred_element_type=jnp.float32)

    def loop(first, n, count, kt):
        def body(w, c):
            m = first + w * n
            probs(scores(m, n, kt), kt)
            grads(m, n, kt)
            return c

        lax.fori_loop(0, count, body, 0)

    n_main = n_items // MAIN
    loop(0, MAIN, n_main, KT)
    loop(n_main * MAIN, TAIL, (n_items - n_main * MAIN + TAIL - 1) // TAIL, KT)
    n_main = n_small // MAIN_SMALL
    loop(cap, MAIN_SMALL, n_main, SMALL)
    loop(cap + n_main * MAIN_SMALL, TAIL, (n_small - n_main * MAIN_SMALL + TAIL - 1) // TAIL, SMALL)
    if nb > 1:
        for ref, (kind, which) in zip(grad_out, outs):
            acc = dk_ref if kind == 'k' else dv_ref
            ref[...] = acc[which[0] * n_keys:(which[-1] + 1) * n_keys, :]
    if last:
        core = lax.rem(me, 2)
        mine = pl.multiple_of(core * half, half)
        theirs = pl.multiple_of((1 - core) * half, half)

        def put(t, c):
            dq_out[0][t] = dq_ref[t, :, pl.ds(mine, half)]
            dq_out[1][t] = dq_ref[t, :, pl.ds(theirs, half)]
            return c

        lax.fori_loop(0, n_sub, put, 0)


def solution(mesh):
    cp = mesh.shape['cp']
    q_spec = P(None, 'cp', 'tp', None)
    lse_spec = P(None, 'cp', 'tp')
    kv_spec = P('cp', 'tp', None)

    def swap(x, bits):
        return lax.ppermute(x, 'cp', [(i, i ^ bits) for i in range(cp)])

    def local_backward(query, out_act, out_grad, row_lse, key_act, value_act, doc_ids):
        n_sub, loc, heads, d = query.shape
        blk = key_act.shape[0]
        n_keys = blk * cp
        half = loc * heads
        sub_len = loc * cp
        pre = n_keys - n_sub * sub_len
        scale = d ** -0.5
        f32, bf16, i32 = jnp.float32, jnp.bfloat16, jnp.int32
        dims = dict(pre=pre, sub_len=sub_len, loc=loc, heads=heads)
        vm = pl.BlockSpec(memory_space=VMEM)
        sm = pl.BlockSpec(memory_space=SMEM)
        hbm = pl.BlockSpec(memory_space=pltpu.HBM)
        sds = jax.ShapeDtypeStruct
        k_own, v_own = key_act.reshape(blk, d), value_act.reshape(blk, d)
        pad = (n_keys // 128 + 7) // 8 * 8
        acc = sds((n_sub, d, 2 * half), f32)
        dq_half = sds((n_sub, d, half), f32)
        cost = pl.CostEstimate(flops=2 * 10 ** 9, bytes_accessed=10 ** 7, transcendentals=10 ** 6)

        def attend(keys, values, dq, blocks, outs, last=False):
            nb = len(blocks)
            ins = [first, q2, do2, lse2, delta, start, *keys, *values] + ([dq] if dq is not None else [])
            cap = nb * n_sub * (-(-blk // KT) + 1) + TAIL
            kv = (nb * blk, d)
            dq_shapes = (dq_half, dq_half) if last else (acc,)
            scratch = [SMEM((2 * cap,), i32)] * 4 + [VMEM((MAIN, KT, 2 * half), bf16)] * 2 + [VMEM((KT, 2 * half), bf16)]
            scratch += [VMEM((n_sub, d, 2 * half), f32)] if last else []
            scratch += [VMEM(kv, bf16)] * 2 + [VMEM(kv, f32)] * 2 if nb > 1 else []
            return pl.pallas_call(
                functools.partial(attn_kernel, blocks=blocks, n_keys=blk, outs=outs, has_dq=dq is not None, last=last,
                                  scale=scale, blk=blk, **dims),
                out_shape=dq_shapes + tuple(sds((len(w) * blk, d), f32) for _, w in outs),
                in_specs=[sm] + [vm] * (len(ins) - 1), out_specs=(vm,) * (len(dq_shapes) + len(outs)),
                scratch_shapes=scratch,
                compiler_params=pltpu.CompilerParams(vmem_limit_bytes=28 * 2 ** 20),
                cost_estimate=cost, name='attn_bwd')(*ins)

        kx, vx, ky, vy, q2, do2, lse2, delta, start, first = pl.pallas_call(
            functools.partial(prep_kernel, **dims),
            out_shape=tuple([sds((blk, d), bf16)] * 4 + [sds((2, n_sub * half, d), bf16)] * 2 + [sds((2, n_sub, half), f32)] * 2
                            + [sds((2, n_sub, half), i32), sds((8, n_sub), i32)]),
            in_specs=[hbm] * 7, out_specs=(vm,) * 10,
            scratch_shapes=[VMEM((2, n_sub * half, d), bf16), VMEM((2, n_sub, heads, loc), f32), VMEM((pad, 128), i32),
                            pltpu.SemaphoreType.DMA((8,)), pltpu.SemaphoreType.DMA((8,)), pltpu.SemaphoreType.DMA((5,))],
            compiler_params=pltpu.CompilerParams(collective_id=0, has_side_effects=True, vmem_limit_bytes=24 * 2 ** 20),
            name='prep',
        )(*[pltpu.with_memory_space_constraint(x, pltpu.HBM) for x in (
            k_own, v_own, query.reshape(-1, d), out_grad.reshape(-1, d), out_act.reshape(-1, d),
            row_lse.transpose(0, 2, 1), doc_ids.reshape(n_keys // 128, 128))])
        kd = swap(kx, 4)
        vd = swap(vy, 2)
        both = (('k', (0,)), ('v', (0,)))
        four = (('k', (0,)), ('k', (1,)), ('v', (0,)), ('v', (1,)))
        dq, dk_x, dk_y, dv_x, dv_y = attend([kx, ky], [vx, vy], None, ((2,), (4,)), four)
        got_ko = swap(dk_x, 2)
        got_vo = swap(dv_y, 4)
        dq, dk_d, dv_d = attend([kd], [vd], dq, ((2, 4),), both)
        got_ky = swap(dk_d, 2)
        got_vx = swap(dv_d, 4)
        dq_own, dq_other, dk_o, dv_o = attend([k_own], [v_own], dq, ((),), both, last=True)
        last_k = swap(dk_y + got_ky, 4)
        last_v = swap(dv_x + got_vx, 2)
        got_dq = swap(dq_other, 1)
        d_query = pl.pallas_call(
            functools.partial(finish_kernel, scale=scale), out_shape=sds((n_sub * half, d), bf16), in_specs=[vm, vm], out_specs=vm,
            compiler_params=pltpu.CompilerParams(vmem_limit_bytes=28 * 2 ** 20),
            cost_estimate=cost, name='finish_dq')(dq_own, got_dq)
        d_key = (dk_o + got_ko + last_k) * scale
        d_value = dv_o + got_vo + last_v
        return d_query.reshape(query.shape), d_key.reshape(key_act.shape), d_value.reshape(value_act.shape)

    return jax.shard_map(local_backward, mesh=mesh, in_specs=(q_spec, q_spec, q_spec, lse_spec, kv_spec, kv_spec, P()), out_specs=(q_spec, kv_spec, kv_spec), check_vma=False)
```

```python
import functools

import jax
import jax.numpy as jnp
from jax import lax
from jax.experimental import pallas as pl
from jax.experimental.pallas import tpu as pltpu
from jax.sharding import PartitionSpec as P


LOG2E = 1.4426950408889634
NT = (((1,), (1,)), ((), ()))
MESH = pl.DeviceIdType.MESH
VMEM, SMEM = pltpu.VMEM, pltpu.SMEM
HIGHEST = lax.Precision.HIGHEST
KT = 256
SMALL = 128
MAIN, MAIN_SMALL, TAIL = 6, 6, 2


def flip(me, bit):
    return me + bit - 2 * bit * lax.rem(me // bit, 2)


def prep_kernel(k_ref, v_ref, q_ref, do_ref, o_ref, lse_ref, ids_ref,
                kx_ref, vx_ref, ky_ref, vy_ref, q2_ref, do2_ref, lse2_ref, delta_ref, start_ref, first_ref,
                o2_ref, lraw_ref, mark_ref, send_sem, recv_sem, load_sem, *, pre, sub_len, loc, heads):
    me = lax.axis_index('cp')
    core = lax.rem(me, 2)
    nx, ny, partner = flip(me, 2), flip(me, 4), flip(me, 1)
    barrier = pltpu.get_barrier_semaphore()
    for other in (nx, ny, partner):
        pl.semaphore_signal(barrier, inc=1, device_id={'cp': other}, device_id_type=MESH)
    pl.semaphore_wait(barrier, 3)
    pairs = [(do_ref, do2_ref), (o_ref, o2_ref), (lse_ref, lraw_ref), (q_ref, q2_ref)]
    moves = [(s, r.at[core], partner) for s, r in pairs]
    moves += [(k_ref, kx_ref, nx), (v_ref, vy_ref, ny), (v_ref, vx_ref, nx), (k_ref, ky_ref, ny)]
    sends = [pltpu.make_async_remote_copy(src_ref=s, dst_ref=r, send_sem=send_sem.at[i], recv_sem=recv_sem.at[i],
                                          device_id={'cp': to}, device_id_type=MESH) for i, (s, r, to) in enumerate(moves)]
    loads = [pltpu.make_async_copy(s, r.at[core], load_sem.at[i]) for i, (s, r) in enumerate(pairs)]
    for copy in sends[4:] + sends[:4] + loads:
        copy.start()

    n_rows = ids_ref.shape[0]
    n_sub = lraw_ref.shape[1]
    pad = mark_ref.shape[0]
    load_ids = pltpu.make_async_copy(ids_ref, mark_ref.at[pl.ds(0, n_rows)], load_sem.at[4])
    load_ids.start()
    mark_ref[pl.ds(n_rows, pad - n_rows), :] = jnp.zeros((pad - n_rows, 128), jnp.int32)
    load_ids.wait()
    ids = mark_ref[...]
    lane = lax.broadcasted_iota(jnp.int32, (pad, 128), 1)
    row = lax.broadcasted_iota(jnp.int32, (pad, 128), 0)
    prev = pltpu.roll(ids, 1, axis=1)
    prev = jnp.where(lane == 0, pltpu.roll(prev, 1, axis=0), prev)
    acc = jnp.where(ids != prev, row * 128 + lane, 0)
    for sh in (1, 2, 4, 8, 16, 32, 64):
        acc = jnp.maximum(acc, jnp.where(lane >= sh, pltpu.roll(acc, sh, axis=1), 0))
    carry = jnp.max(acc, axis=1, keepdims=True) + jnp.zeros((pad, 128), jnp.int32)
    carry = jnp.where(row >= 1, pltpu.roll(carry, 1, axis=0), 0)
    sh = 1
    while sh < pad:
        carry = jnp.maximum(carry, jnp.where(row >= sh, pltpu.roll(carry, sh, axis=0), 0))
        sh *= 2
    starts = jnp.maximum(acc, carry).astype(jnp.float32)

    def hdot(a, b, dims=None):
        dims = (((1,), (0,)), ((), ())) if dims is None else dims
        return lax.dot_general(a, b, dims, precision=HIGHEST, preferred_element_type=jnp.float32)

    per = sub_len // 128
    off = (me // 2) * 2 * loc
    r_sub = lax.broadcasted_iota(jnp.int32, (n_sub, pad), 0)
    r_row = lax.broadcasted_iota(jnp.int32, (n_sub, pad), 1)
    pick = jnp.where(r_row == pre // 128 + per * r_sub + off // 128, 1.0, 0.0)
    sub_starts = hdot(pick, starts)
    src = lax.broadcasted_iota(jnp.int32, (128, 128), 0)
    dst = lax.broadcasted_iota(jnp.int32, (128, 128), 1)
    for e in range(2):
        spread = jnp.where(src == lax.rem(off, 128) + e * loc + dst // heads, 1.0, 0.0)
        rows_start = hdot(sub_starts, spread)
        start_ref[e] = rows_start.astype(jnp.int32)
        if e == 0:
            head = jnp.where(lax.broadcasted_iota(jnp.int32, (8, 128), 1) == 0, 1.0, 0.0)
            first_ref[...] = hdot(head, rows_start, NT).astype(jnp.int32)

    def delta_of(e, o_part):
        def body(t, c):
            r0 = pl.multiple_of(t * 128, 128)
            prod = do2_ref[e, pl.ds(r0, 128), :].astype(jnp.float32) * o_part[pl.ds(r0, 128), :].astype(jnp.float32)
            delta_ref[e, pl.ds(t, 1), :] = jnp.sum(prod.T, axis=0, keepdims=True)
            return c

        lax.fori_loop(0, n_sub, body, 0)

    for load in loads:
        load.wait()
    delta_of(core, o2_ref.at[core])
    for copy in sends[:3]:
        copy.wait_recv()
    delta_of(1 - core, o2_ref.at[1 - core])
    tok = lax.broadcasted_iota(jnp.int32, (loc, 128), 0)
    tok_lane = lax.broadcasted_iota(jnp.int32, (loc, 128), 1)
    tok_spread = jnp.where(tok == tok_lane // heads, 1.0, 0.0)
    head_of = lax.broadcasted_iota(jnp.int32, (n_sub * heads, 128), 0)
    head_lane = lax.broadcasted_iota(jnp.int32, (n_sub * heads, 128), 1)
    own_head = lax.rem(head_of, heads) == lax.rem(head_lane, heads)
    g_sub = lax.broadcasted_iota(jnp.int32, (n_sub, n_sub * heads), 0)
    g_row = lax.broadcasted_iota(jnp.int32, (n_sub, n_sub * heads), 1)
    group = jnp.where(g_row // heads == g_sub, 1.0, 0.0)
    for e in range(2):
        wide = hdot(lraw_ref[e].reshape(n_sub * heads, loc), tok_spread)
        lse2_ref[e] = hdot(group, jnp.where(own_head, wide, 0.0)) * LOG2E
    for copy in sends[3:]:
        copy.wait_recv()
    for copy in sends:
        copy.wait_send()


def finish_kernel(own_ref, got_ref, out_ref, *, scale):
    half = own_ref.shape[2]

    step = 4

    def put(i, c):
        for u in range(step):
            t = i * step + u
            total = (own_ref[t] + got_ref[t]) * scale
            out_ref[pl.ds(pl.multiple_of(t * half, half), half), :] = total.T.astype(jnp.bfloat16)
        return c

    lax.fori_loop(0, own_ref.shape[0] // step, put, 0)


def attn_kernel(*refs, blocks, row0, n_keys, outs, n_prev, has_dq, last, scale, blk, pre, sub_len, loc, heads):
    first_ref, q_ref, do_ref, lse_ref, delta_ref, start_ref = refs[:6]
    nb = len(blocks)
    k_in, v_in, refs = refs[6:6 + nb], refs[6 + nb:6 + 2 * nb], refs[6 + 2 * nb:]
    if has_dq:
        dq_in, refs = refs[0], refs[1:]
    prev, refs = refs[:n_prev], refs[n_prev:]
    n_dq = 2 if last else 1
    dq_out, grad_out, refs = refs[:n_dq], refs[n_dq:n_dq + len(outs)], refs[n_dq + len(outs):]
    it_t, it_k, it_lo, it_base, p_ref, ds_ref, kpos_ref, refs = *refs[:7], refs[7:]
    if last:
        dq_ref, refs = refs[0], refs[1:]
    else:
        dq_ref = dq_out[0]
    if nb == 1:
        k_ref, v_ref, dk_ref, dv_ref = k_in[0], v_in[0], grad_out[0], grad_out[1]
    else:
        k_ref, v_ref, dk_ref, dv_ref = refs
    me = lax.axis_index('cp')
    n_sub, half = lse_ref.shape[1], lse_ref.shape[2]
    rows = 2 * half
    pos0 = pre + (me // 2) * 2 * loc
    if nb > 1:
        for b in range(nb):
            k_ref[b * n_keys:(b + 1) * n_keys, :] = k_in[b][row0:row0 + n_keys, :]
            v_ref[b * n_keys:(b + 1) * n_keys, :] = v_in[b][row0:row0 + n_keys, :]
    dk_ref[...] = jnp.zeros_like(dk_ref)
    dv_ref[...] = jnp.zeros_like(dv_ref)
    if has_dq:
        dq_ref[...] = dq_in[...]
    else:
        dq_ref[...] = jnp.zeros_like(dq_ref)

    cap = it_t.shape[0] // 2

    def put_item(m, t, b, row, lo, blo, kt):
        it_t[m] = t
        it_k[m] = b * n_keys + jnp.minimum(row, n_keys - kt)
        it_lo[m] = lo
        it_base[m] = blo - b * n_keys

    n_items, n_small = 0, 0
    for b, bits in enumerate(blocks):
        owner = me
        for bit in bits:
            owner = flip(owner, bit)
        blo = owner * blk + row0

        def more(c, blo=blo):
            return (c[0] < n_sub) & (first_ref[0, jnp.minimum(c[0], n_sub - 1)] < blo + n_keys)

        def add_tile(c, b=b, blo=blo):
            t, n, ns = c
            lo = jnp.maximum(first_ref[0, t], blo)
            hi = jnp.minimum(pos0 + t * sub_len + 2 * loc - 1, blo + n_keys - 1)
            off = (lo - blo) // 16 * 16
            length = hi - blo - off + 1
            full = length // KT
            rest = length - full * KT
            cnt = full + jnp.where(rest > SMALL, 1, 0)

            def add_item(i, m):
                put_item(m, t, b, off + i * KT, blo + off + i * KT, blo, KT)
                return m + 1

            put_item(cap + ns, t, b, off + full * KT, blo + off + full * KT, blo, SMALL)
            ns = ns + jnp.where((rest > 0) & (rest <= SMALL), 1, 0)
            return t + 1, lax.fori_loop(0, cnt, add_item, n), ns

        t_first = jnp.maximum(blo - pos0 - 2 * loc + sub_len, 0) // sub_len
        _, n_items, n_small = lax.while_loop(more, add_tile, (t_first, n_items, n_small))
    for n in (n_items, cap + n_small):
        put_item(n, 0, 0, 0, 1 << 30, 0, KT)

    def two(ref, t):
        return jnp.concatenate([ref[0, pl.ds(t, 1), :], ref[1, pl.ds(t, 1), :]], axis=1)

    lane = lax.broadcasted_iota(jnp.int32, (1, rows), 1)
    zero = jnp.zeros((16, rows), jnp.bfloat16)
    kpos_ref[...] = lax.broadcasted_iota(jnp.int32, (KT, rows), 0).astype(jnp.float32).astype(jnp.bfloat16)

    def item(m):
        t = it_t[m]
        k0 = pl.multiple_of(it_k[m], 16)
        r0 = pl.multiple_of(t * half, half)
        q = jnp.concatenate([q_ref[0, pl.ds(r0, half), :], q_ref[1, pl.ds(r0, half), :]], axis=0)
        do = jnp.concatenate([do_ref[0, pl.ds(r0, half), :], do_ref[1, pl.ds(r0, half), :]], axis=0)
        return t, k0, q, do

    def scores(first, n, kt):
        out = []
        for u in range(n):
            m = first + u
            t, k0, q, do = item(m)
            s = lax.dot_general(k_ref[pl.ds(k0, kt), :], q, NT, preferred_element_type=jnp.float32)
            dp = lax.dot_general(v_ref[pl.ds(k0, kt), :], do, NT, preferred_element_type=jnp.float32)
            lo = jnp.maximum(two(start_ref, t), it_lo[m]) - (k0 + it_base[m])
            qpos = lane // heads + (pos0 + t * sub_len - k0 - it_base[m])
            lo = packed(jnp.clip(lo, 0, KT))
            qpos = packed(jnp.clip(qpos, -1, KT))
            out.append((s, dp, lo, qpos, two(lse_ref, t), two(delta_ref, t)))
        return out

    def packed(x):
        return jnp.broadcast_to(x.astype(jnp.float32), (16, rows)).astype(jnp.bfloat16)

    def probs(parts, kt):
        for u in range(len(parts)):
            s, dp, lo, qpos, lse, delta = parts[u]
            for g in range(kt // 16):
                r = slice(16 * g, 16 * g + 16)
                kpos = kpos_ref[r, :]
                allowed = (kpos >= lo) & (kpos <= qpos)
                p = jnp.exp2(s[r, :] * (scale * LOG2E) - lse)
                ds = p * (dp[r, :] - delta)
                p_ref[u, r, :] = jnp.where(allowed, p.astype(jnp.bfloat16), zero)
                ds_ref[u, r, :] = jnp.where(allowed, ds.astype(jnp.bfloat16), zero)

    def grads(first, n, kt):
        for u in range(n):
            t, k0, q, do = item(first + u)
            p, ds = p_ref[u, :kt, :], ds_ref[u, :kt, :]
            dv_ref[pl.ds(k0, kt), :] += jnp.dot(p, do, preferred_element_type=jnp.float32)
            dk_ref[pl.ds(k0, kt), :] += jnp.dot(ds, q, preferred_element_type=jnp.float32)
            dq_ref[t] += jnp.dot(k_ref[pl.ds(k0, kt), :].T, ds, preferred_element_type=jnp.float32)

    def loop(first, n, count, kt):
        def body(w, c):
            m = first + w * n
            probs(scores(m, n, kt), kt)
            grads(m, n, kt)
            return c

        lax.fori_loop(0, count, body, 0)

    n_main = n_items // MAIN
    loop(0, MAIN, n_main, KT)
    loop(n_main * MAIN, TAIL, (n_items - n_main * MAIN + TAIL - 1) // TAIL, KT)
    n_main = n_small // MAIN_SMALL
    loop(cap, MAIN_SMALL, n_main, SMALL)
    loop(cap + n_main * MAIN_SMALL, TAIL, (n_small - n_main * MAIN_SMALL + TAIL - 1) // TAIL, SMALL)
    if nb > 1:
        for ref, (kind, b, i) in zip(grad_out, outs):
            acc = dk_ref if kind == 'k' else dv_ref
            if i is None:
                ref[...] = acc[b * n_keys:(b + 1) * n_keys, :]
            else:
                ref[0:row0, :] = prev[i][...]
                ref[row0:row0 + n_keys, :] = acc[b * n_keys:(b + 1) * n_keys, :]
    if last:
        core = lax.rem(me, 2)
        mine = pl.multiple_of(core * half, half)
        theirs = pl.multiple_of((1 - core) * half, half)

        def put(t, c):
            dq_out[0][t] = dq_ref[t, :, pl.ds(mine, half)]
            dq_out[1][t] = dq_ref[t, :, pl.ds(theirs, half)]
            return c

        lax.fori_loop(0, n_sub, put, 0)


def solution(mesh):
    cp = mesh.shape['cp']
    q_spec = P(None, 'cp', 'tp', None)
    lse_spec = P(None, 'cp', 'tp')
    kv_spec = P('cp', 'tp', None)

    def swap(x, bits):
        return lax.ppermute(x, 'cp', [(i, i ^ bits) for i in range(cp)])

    def local_backward(query, out_act, out_grad, row_lse, key_act, value_act, doc_ids):
        n_sub, loc, heads, d = query.shape
        blk = key_act.shape[0]
        n_keys = blk * cp
        half = loc * heads
        sub_len = loc * cp
        pre = n_keys - n_sub * sub_len
        scale = d ** -0.5
        f32, bf16, i32 = jnp.float32, jnp.bfloat16, jnp.int32
        dims = dict(pre=pre, sub_len=sub_len, loc=loc, heads=heads)
        vm = pl.BlockSpec(memory_space=VMEM)
        sm = pl.BlockSpec(memory_space=SMEM)
        hbm = pl.BlockSpec(memory_space=pltpu.HBM)
        sds = jax.ShapeDtypeStruct
        k_own, v_own = key_act.reshape(blk, d), value_act.reshape(blk, d)
        pad = (n_keys // 128 + 7) // 8 * 8
        acc = sds((n_sub, d, 2 * half), f32)
        dq_half = sds((n_sub, d, half), f32)
        cost = pl.CostEstimate(flops=2 * 10 ** 9, bytes_accessed=10 ** 7, transcendentals=10 ** 6)

        def attend(keys, values, dq, blocks, outs, row0=0, n_rows=blk, prev=(), last=False):
            nb = len(blocks)
            ins = [first, q2, do2, lse2, delta, start, *keys, *values] + ([dq] if dq is not None else []) + list(prev)
            cap = nb * n_sub * (-(-n_rows // KT) + 1) + TAIL
            kv = (nb * n_rows, d)
            dq_shapes = (dq_half, dq_half) if last else (acc,)
            scratch = [SMEM((2 * cap,), i32)] * 4 + [VMEM((MAIN, KT, 2 * half), bf16)] * 2 + [VMEM((KT, 2 * half), bf16)]
            scratch += [VMEM((n_sub, d, 2 * half), f32)] if last else []
            scratch += [VMEM(kv, bf16)] * 2 + [VMEM(kv, f32)] * 2 if nb > 1 else []
            return pl.pallas_call(
                functools.partial(attn_kernel, blocks=blocks, row0=row0, n_keys=n_rows, outs=outs, n_prev=len(prev),
                                  has_dq=dq is not None, last=last,
                                  scale=scale, blk=blk, **dims),
                out_shape=dq_shapes + tuple(sds((n_rows if i is None else row0 + n_rows, d), f32) for _, _, i in outs),
                in_specs=[sm] + [vm] * (len(ins) - 1), out_specs=(vm,) * (len(dq_shapes) + len(outs)),
                scratch_shapes=scratch,
                compiler_params=pltpu.CompilerParams(vmem_limit_bytes=28 * 2 ** 20),
                cost_estimate=cost, name='attn_bwd')(*ins)

        kx, vx, ky, vy, q2, do2, lse2, delta, start, first = pl.pallas_call(
            functools.partial(prep_kernel, **dims),
            out_shape=tuple([sds((blk, d), bf16)] * 4 + [sds((2, n_sub * half, d), bf16)] * 2 + [sds((2, n_sub, half), f32)] * 2
                            + [sds((2, n_sub, half), i32), sds((8, n_sub), i32)]),
            in_specs=[hbm] * 7, out_specs=(vm,) * 10,
            scratch_shapes=[VMEM((2, n_sub * half, d), bf16), VMEM((2, n_sub, heads, loc), f32), VMEM((pad, 128), i32),
                            pltpu.SemaphoreType.DMA((8,)), pltpu.SemaphoreType.DMA((8,)), pltpu.SemaphoreType.DMA((5,))],
            compiler_params=pltpu.CompilerParams(collective_id=0, has_side_effects=True, vmem_limit_bytes=24 * 2 ** 20),
            name='prep',
        )(*[pltpu.with_memory_space_constraint(x, pltpu.HBM) for x in (
            k_own, v_own, query.reshape(-1, d), out_grad.reshape(-1, d), out_act.reshape(-1, d),
            row_lse.transpose(0, 2, 1), doc_ids.reshape(n_keys // 128, 128))])
        kd = swap(kx, 4)
        vd = swap(vy, 2)
        both = (('k', 0, None), ('v', 0, None))
        sides = ((2,), (4,))
        cut = blk // KT // 2 * KT
        four = (('k', 0, None), ('v', 1, None), ('k', 1, None), ('v', 0, None))
        dq, dk_xa, dv_ya, dk_ya, dv_xa = attend([kx, ky], [vx, vy], None, sides, four, 0, cut)
        got_ka = swap(dk_xa, 2)
        got_va = swap(dv_ya, 4)
        dq, dk_d, dv_d = attend([kd], [vd], dq, ((2, 4),), both)
        got_ky = swap(dk_d, 2)
        got_vx = swap(dv_d, 4)
        four = (('k', 0, None), ('v', 1, None), ('k', 1, 0), ('v', 0, 1))
        dq, dk_xb, dv_yb, dk_y, dv_x = attend([kx, ky], [vx, vy], dq, sides, four, cut, blk - cut, (dk_ya, dv_xa))
        got_kb = swap(dk_xb, 2)
        got_vb = swap(dv_yb, 4)
        last_k = swap(dk_y + got_ky, 4)
        last_v = swap(dv_x + got_vx, 2)
        dq_own, dq_other, dk_o, dv_o = attend([k_own], [v_own], dq, ((),), both, last=True)
        got_dq = swap(dq_other, 1)
        d_query = pl.pallas_call(
            functools.partial(finish_kernel, scale=scale), out_shape=sds((n_sub * half, d), bf16), in_specs=[vm, vm], out_specs=vm,
            compiler_params=pltpu.CompilerParams(vmem_limit_bytes=28 * 2 ** 20),
            cost_estimate=cost, name='finish_dq')(dq_own, got_dq)
        d_key = (dk_o + jnp.concatenate([got_ka, got_kb]) + last_k) * scale
        d_value = dv_o + jnp.concatenate([got_va, got_vb]) + last_v
        return d_query.reshape(query.shape), d_key.reshape(key_act.shape), d_value.reshape(value_act.shape)

    return jax.shard_map(local_backward, mesh=mesh, in_specs=(q_spec, q_spec, q_spec, lse_spec, kv_spec, kv_spec, P()), out_specs=(q_spec, kv_spec, kv_spec), check_vma=False)
```

```python
import functools

import jax
import jax.numpy as jnp
from jax import lax
from jax.experimental import pallas as pl
from jax.experimental.pallas import tpu as pltpu
from jax.sharding import PartitionSpec as P


LOG2E = 1.4426950408889634
NT = (((1,), (1,)), ((), ()))
MESH = pl.DeviceIdType.MESH
VMEM, SMEM = pltpu.VMEM, pltpu.SMEM
HIGHEST = lax.Precision.HIGHEST
KT = 256
SMALL = 128
MAIN, MAIN_SMALL, TAIL = 6, 6, 2


def flip(me, bit):
    return me + bit - 2 * bit * lax.rem(me // bit, 2)


def prep_kernel(k_ref, v_ref, q_ref, do_ref, o_ref, lse_ref, ids_ref,
                kx_ref, vx_ref, ky_ref, vy_ref, q2_ref, do2_ref, lse2_ref, delta_ref, start_ref, first_ref,
                o2_ref, lraw_ref, mark_ref, send_sem, recv_sem, load_sem, *, pre, sub_len, loc, heads):
    me = lax.axis_index('cp')
    core = lax.rem(me, 2)
    nx, ny, partner = flip(me, 2), flip(me, 4), flip(me, 1)
    barrier = pltpu.get_barrier_semaphore()
    for other in (nx, ny, partner):
        pl.semaphore_signal(barrier, inc=1, device_id={'cp': other}, device_id_type=MESH)
    pl.semaphore_wait(barrier, 3)
    pairs = [(do_ref, do2_ref), (o_ref, o2_ref), (lse_ref, lraw_ref), (q_ref, q2_ref)]
    moves = [(s, r.at[core], partner) for s, r in pairs]
    moves += [(k_ref, kx_ref, nx), (v_ref, vy_ref, ny), (v_ref, vx_ref, nx), (k_ref, ky_ref, ny)]
    sends = [pltpu.make_async_remote_copy(src_ref=s, dst_ref=r, send_sem=send_sem.at[i], recv_sem=recv_sem.at[i],
                                          device_id={'cp': to}, device_id_type=MESH) for i, (s, r, to) in enumerate(moves)]
    loads = [pltpu.make_async_copy(s, r.at[core], load_sem.at[i]) for i, (s, r) in enumerate(pairs)]
    for copy in sends[4:] + sends[:4] + loads:
        copy.start()

    n_rows = ids_ref.shape[0]
    n_sub = lraw_ref.shape[1]
    pad = mark_ref.shape[0]
    load_ids = pltpu.make_async_copy(ids_ref, mark_ref.at[pl.ds(0, n_rows)], load_sem.at[4])
    load_ids.start()
    mark_ref[pl.ds(n_rows, pad - n_rows), :] = jnp.zeros((pad - n_rows, 128), jnp.int32)
    load_ids.wait()
    ids = mark_ref[...]
    lane = lax.broadcasted_iota(jnp.int32, (pad, 128), 1)
    row = lax.broadcasted_iota(jnp.int32, (pad, 128), 0)
    prev = pltpu.roll(ids, 1, axis=1)
    prev = jnp.where(lane == 0, pltpu.roll(prev, 1, axis=0), prev)
    acc = jnp.where(ids != prev, row * 128 + lane, 0)
    for sh in (1, 2, 4, 8, 16, 32, 64):
        acc = jnp.maximum(acc, jnp.where(lane >= sh, pltpu.roll(acc, sh, axis=1), 0))
    carry = jnp.max(acc, axis=1, keepdims=True) + jnp.zeros((pad, 128), jnp.int32)
    carry = jnp.where(row >= 1, pltpu.roll(carry, 1, axis=0), 0)
    sh = 1
    while sh < pad:
        carry = jnp.maximum(carry, jnp.where(row >= sh, pltpu.roll(carry, sh, axis=0), 0))
        sh *= 2
    starts = jnp.maximum(acc, carry).astype(jnp.float32)

    def hdot(a, b, dims=None):
        dims = (((1,), (0,)), ((), ())) if dims is None else dims
        return lax.dot_general(a, b, dims, precision=HIGHEST, preferred_element_type=jnp.float32)

    per = sub_len // 128
    off = (me // 2) * 2 * loc
    r_sub = lax.broadcasted_iota(jnp.int32, (n_sub, pad), 0)
    r_row = lax.broadcasted_iota(jnp.int32, (n_sub, pad), 1)
    pick = jnp.where(r_row == pre // 128 + per * r_sub + off // 128, 1.0, 0.0)
    sub_starts = hdot(pick, starts)
    src = lax.broadcasted_iota(jnp.int32, (128, 128), 0)
    dst = lax.broadcasted_iota(jnp.int32, (128, 128), 1)
    for e in range(2):
        spread = jnp.where(src == lax.rem(off, 128) + e * loc + dst // heads, 1.0, 0.0)
        rows_start = hdot(sub_starts, spread)
        start_ref[e] = rows_start.astype(jnp.int32)
        if e == 0:
            head = jnp.where(lax.broadcasted_iota(jnp.int32, (8, 128), 1) == 0, 1.0, 0.0)
            first_ref[...] = hdot(head, rows_start, NT).astype(jnp.int32)

    def delta_of(e, o_part):
        def body(t, c):
            r0 = pl.multiple_of(t * 128, 128)
            prod = do2_ref[e, pl.ds(r0, 128), :].astype(jnp.float32) * o_part[pl.ds(r0, 128), :].astype(jnp.float32)
            delta_ref[e, pl.ds(t, 1), :] = jnp.sum(prod.T, axis=0, keepdims=True)
            return c

        lax.fori_loop(0, n_sub, body, 0)

    for load in loads:
        load.wait()
    delta_of(core, o2_ref.at[core])
    for copy in sends[:3]:
        copy.wait_recv()
    delta_of(1 - core, o2_ref.at[1 - core])
    tok = lax.broadcasted_iota(jnp.int32, (loc, 128), 0)
    tok_lane = lax.broadcasted_iota(jnp.int32, (loc, 128), 1)
    tok_spread = jnp.where(tok == tok_lane // heads, 1.0, 0.0)
    head_of = lax.broadcasted_iota(jnp.int32, (n_sub * heads, 128), 0)
    head_lane = lax.broadcasted_iota(jnp.int32, (n_sub * heads, 128), 1)
    own_head = lax.rem(head_of, heads) == lax.rem(head_lane, heads)
    g_sub = lax.broadcasted_iota(jnp.int32, (n_sub, n_sub * heads), 0)
    g_row = lax.broadcasted_iota(jnp.int32, (n_sub, n_sub * heads), 1)
    group = jnp.where(g_row // heads == g_sub, 1.0, 0.0)
    for e in range(2):
        wide = hdot(lraw_ref[e].reshape(n_sub * heads, loc), tok_spread)
        lse2_ref[e] = hdot(group, jnp.where(own_head, wide, 0.0)) * LOG2E
    for copy in sends[3:]:
        copy.wait_recv()
    for copy in sends:
        copy.wait_send()


def finish_kernel(own_ref, got_ref, out_ref, *, scale):
    half = own_ref.shape[2]

    step = 4

    def put(i, c):
        for u in range(step):
            t = i * step + u
            total = (own_ref[t] + got_ref[t]) * scale
            out_ref[pl.ds(pl.multiple_of(t * half, half), half), :] = total.T.astype(jnp.bfloat16)
        return c

    lax.fori_loop(0, own_ref.shape[0] // step, put, 0)


def sum_kernel(dk_ref, ka_ref, kb_ref, lk_ref, dv_ref, va_ref, vb_ref, lv_ref, dk_out, dv_out, sum_ref, sem, *, scale, cut):
    n = dk_ref.shape[0]
    copies = []
    for i, (own, a, b, end, out, mul) in enumerate([(dk_ref, ka_ref, kb_ref, lk_ref, dk_out, scale), (dv_ref, va_ref, vb_ref, lv_ref, dv_out, 1.0)]):
        sum_ref[i, 0:cut, :] = (own[0:cut, :] + a[...] + end[0:cut, :]) * mul
        sum_ref[i, cut:n, :] = (own[cut:n, :] + b[...] + end[cut:n, :]) * mul
        copies.append(pltpu.make_async_copy(sum_ref.at[i], out, sem.at[i]))
        copies[-1].start()
    for copy in copies:
        copy.wait()


def attn_kernel(*refs, blocks, row0, n_keys, outs, n_prev, has_dq, last, scale, blk, pre, sub_len, loc, heads):
    first_ref, q_ref, do_ref, lse_ref, delta_ref, start_ref = refs[:6]
    nb = len(blocks)
    k_in, v_in, refs = refs[6:6 + nb], refs[6 + nb:6 + 2 * nb], refs[6 + 2 * nb:]
    if has_dq:
        dq_in, refs = refs[0], refs[1:]
    prev, refs = refs[:n_prev], refs[n_prev:]
    n_dq = 2 if last else 1
    dq_out, grad_out, refs = refs[:n_dq], refs[n_dq:n_dq + len(outs)], refs[n_dq + len(outs):]
    it_t, it_k, it_lo, it_base, p_ref, ds_ref, kpos_ref, refs = *refs[:7], refs[7:]
    if last:
        dq_ref, refs = refs[0], refs[1:]
    else:
        dq_ref = dq_out[0]
    if nb == 1:
        k_ref, v_ref, dk_ref, dv_ref = k_in[0], v_in[0], grad_out[0], grad_out[1]
    else:
        k_ref, v_ref, dk_ref, dv_ref = refs
    me = lax.axis_index('cp')
    n_sub, half = lse_ref.shape[1], lse_ref.shape[2]
    rows = 2 * half
    pos0 = pre + (me // 2) * 2 * loc
    if nb > 1:
        for b in range(nb):
            k_ref[b * n_keys:(b + 1) * n_keys, :] = k_in[b][row0:row0 + n_keys, :]
            v_ref[b * n_keys:(b + 1) * n_keys, :] = v_in[b][row0:row0 + n_keys, :]
    dk_ref[...] = jnp.zeros_like(dk_ref)
    dv_ref[...] = jnp.zeros_like(dv_ref)
    if last:
        dq_ref[...] = dq_in[...]
    elif not has_dq:
        dq_ref[...] = jnp.zeros_like(dq_ref)

    cap = it_t.shape[0] // 2

    def put_item(m, t, b, row, lo, blo, kt):
        it_t[m] = t
        it_k[m] = b * n_keys + jnp.minimum(row, n_keys - kt)
        it_lo[m] = lo
        it_base[m] = blo - b * n_keys

    n_items, n_small = 0, 0
    for b, bits in enumerate(blocks):
        owner = me
        for bit in bits:
            owner = flip(owner, bit)
        blo = owner * blk + row0

        def more(c, blo=blo):
            return (c[0] < n_sub) & (first_ref[0, jnp.minimum(c[0], n_sub - 1)] < blo + n_keys)

        def add_tile(c, b=b, blo=blo):
            t, n, ns = c
            lo = jnp.maximum(first_ref[0, t], blo)
            hi = jnp.minimum(pos0 + t * sub_len + 2 * loc - 1, blo + n_keys - 1)
            off = (lo - blo) // 16 * 16
            length = hi - blo - off + 1
            full = length // KT
            rest = length - full * KT
            cnt = full + jnp.where(rest > SMALL, 1, 0)

            def add_item(i, m):
                put_item(m, t, b, off + i * KT, blo + off + i * KT, blo, KT)
                return m + 1

            put_item(cap + ns, t, b, off + full * KT, blo + off + full * KT, blo, SMALL)
            ns = ns + jnp.where((rest > 0) & (rest <= SMALL), 1, 0)
            return t + 1, lax.fori_loop(0, cnt, add_item, n), ns

        t_first = jnp.maximum(blo - pos0 - 2 * loc + sub_len, 0) // sub_len
        _, n_items, n_small = lax.while_loop(more, add_tile, (t_first, n_items, n_small))
    for n in (n_items, cap + n_small):
        put_item(n, 0, 0, 0, 1 << 30, 0, KT)

    def two(ref, t):
        return jnp.concatenate([ref[0, pl.ds(t, 1), :], ref[1, pl.ds(t, 1), :]], axis=1)

    lane = lax.broadcasted_iota(jnp.int32, (1, rows), 1)
    zero = jnp.zeros((16, rows), jnp.bfloat16)
    kpos_ref[...] = lax.broadcasted_iota(jnp.int32, (KT, rows), 0).astype(jnp.float32).astype(jnp.bfloat16)

    def item(m):
        t = it_t[m]
        k0 = pl.multiple_of(it_k[m], 16)
        r0 = pl.multiple_of(t * half, half)
        q = jnp.concatenate([q_ref[0, pl.ds(r0, half), :], q_ref[1, pl.ds(r0, half), :]], axis=0)
        do = jnp.concatenate([do_ref[0, pl.ds(r0, half), :], do_ref[1, pl.ds(r0, half), :]], axis=0)
        return t, k0, q, do

    def scores(first, n, kt):
        out = []
        for u in range(n):
            m = first + u
            t, k0, q, do = item(m)
            s = lax.dot_general(k_ref[pl.ds(k0, kt), :], q, NT, preferred_element_type=jnp.float32)
            dp = lax.dot_general(v_ref[pl.ds(k0, kt), :], do, NT, preferred_element_type=jnp.float32)
            lo = jnp.maximum(two(start_ref, t), it_lo[m]) - (k0 + it_base[m])
            qpos = lane // heads + (pos0 + t * sub_len - k0 - it_base[m])
            lo = packed(jnp.clip(lo, 0, KT))
            qpos = packed(jnp.clip(qpos, -1, KT))
            out.append((s, dp, lo, qpos, two(lse_ref, t), two(delta_ref, t)))
        return out

    def packed(x):
        return jnp.broadcast_to(x.astype(jnp.float32), (16, rows)).astype(jnp.bfloat16)

    def probs(parts, kt):
        for u in range(len(parts)):
            s, dp, lo, qpos, lse, delta = parts[u]
            for g in range(kt // 16):
                r = slice(16 * g, 16 * g + 16)
                kpos = kpos_ref[r, :]
                allowed = (kpos >= lo) & (kpos <= qpos)
                p = jnp.exp2(s[r, :] * (scale * LOG2E) - lse)
                ds = p * (dp[r, :] - delta)
                p_ref[u, r, :] = jnp.where(allowed, p.astype(jnp.bfloat16), zero)
                ds_ref[u, r, :] = jnp.where(allowed, ds.astype(jnp.bfloat16), zero)

    def grads(first, n, kt):
        for u in range(n):
            t, k0, q, do = item(first + u)
            p, ds = p_ref[u, :kt, :], ds_ref[u, :kt, :]
            dv_ref[pl.ds(k0, kt), :] += jnp.dot(p, do, preferred_element_type=jnp.float32)
            dk_ref[pl.ds(k0, kt), :] += jnp.dot(ds, q, preferred_element_type=jnp.float32)
            dq_ref[t] += jnp.dot(k_ref[pl.ds(k0, kt), :].T, ds, preferred_element_type=jnp.float32)

    def loop(first, n, count, kt):
        def body(w, c):
            m = first + w * n
            probs(scores(m, n, kt), kt)
            grads(m, n, kt)
            return c

        lax.fori_loop(0, count, body, 0)

    n_main = n_items // MAIN
    loop(0, MAIN, n_main, KT)
    loop(n_main * MAIN, TAIL, (n_items - n_main * MAIN + TAIL - 1) // TAIL, KT)
    n_main = n_small // MAIN_SMALL
    loop(cap, MAIN_SMALL, n_main, SMALL)
    loop(cap + n_main * MAIN_SMALL, TAIL, (n_small - n_main * MAIN_SMALL + TAIL - 1) // TAIL, SMALL)
    if nb > 1:
        for ref, (kind, b, i) in zip(grad_out, outs):
            acc = dk_ref if kind == 'k' else dv_ref
            if i is None:
                ref[...] = acc[b * n_keys:(b + 1) * n_keys, :]
            else:
                ref[0:row0, :] = prev[i][...]
                ref[row0:row0 + n_keys, :] = acc[b * n_keys:(b + 1) * n_keys, :]
    if last:
        core = lax.rem(me, 2)
        mine = pl.multiple_of(core * half, half)
        theirs = pl.multiple_of((1 - core) * half, half)

        def put(t, c):
            dq_out[0][t] = dq_ref[t, :, pl.ds(mine, half)]
            dq_out[1][t] = dq_ref[t, :, pl.ds(theirs, half)]
            return c

        lax.fori_loop(0, n_sub, put, 0)


def solution(mesh):
    cp = mesh.shape['cp']
    q_spec = P(None, 'cp', 'tp', None)
    lse_spec = P(None, 'cp', 'tp')
    kv_spec = P('cp', 'tp', None)

    def swap(x, bits):
        return lax.ppermute(x, 'cp', [(i, i ^ bits) for i in range(cp)])

    def local_backward(query, out_act, out_grad, row_lse, key_act, value_act, doc_ids):
        n_sub, loc, heads, d = query.shape
        blk = key_act.shape[0]
        n_keys = blk * cp
        half = loc * heads
        sub_len = loc * cp
        pre = n_keys - n_sub * sub_len
        scale = d ** -0.5
        f32, bf16, i32 = jnp.float32, jnp.bfloat16, jnp.int32
        dims = dict(pre=pre, sub_len=sub_len, loc=loc, heads=heads)
        vm = pl.BlockSpec(memory_space=VMEM)
        sm = pl.BlockSpec(memory_space=SMEM)
        hbm = pl.BlockSpec(memory_space=pltpu.HBM)
        sds = jax.ShapeDtypeStruct
        k_own, v_own = key_act.reshape(blk, d), value_act.reshape(blk, d)
        pad = (n_keys // 128 + 7) // 8 * 8
        acc = sds((n_sub, d, 2 * half), f32)
        kv_out = sds((blk, d), f32)
        dq_half = sds((n_sub, d, half), f32)
        cost = pl.CostEstimate(flops=2 * 10 ** 9, bytes_accessed=10 ** 7, transcendentals=10 ** 6)

        def attend(keys, values, dq, blocks, outs, row0=0, n_rows=blk, prev=(), last=False):
            nb = len(blocks)
            ins = [first, q2, do2, lse2, delta, start, *keys, *values] + ([dq] if dq is not None else []) + list(prev)
            cap = nb * n_sub * (-(-n_rows // KT) + 1) + TAIL
            kv = (nb * n_rows, d)
            dq_shapes = (dq_half, dq_half) if last else (acc,)
            scratch = [SMEM((2 * cap,), i32)] * 4 + [VMEM((MAIN, KT, 2 * half), bf16)] * 2 + [VMEM((KT, 2 * half), bf16)]
            scratch += [VMEM((n_sub, d, 2 * half), f32)] if last else []
            scratch += [VMEM(kv, bf16)] * 2 + [VMEM(kv, f32)] * 2 if nb > 1 else []
            return pl.pallas_call(
                functools.partial(attn_kernel, blocks=blocks, row0=row0, n_keys=n_rows, outs=outs, n_prev=len(prev),
                                  has_dq=dq is not None, last=last,
                                  scale=scale, blk=blk, **dims),
                out_shape=dq_shapes + tuple(sds((n_rows if i is None else row0 + n_rows, d), f32) for _, _, i in outs),
                in_specs=[sm] + [vm] * (len(ins) - 1), out_specs=(vm,) * (len(dq_shapes) + len(outs)),
                scratch_shapes=scratch, input_output_aliases={6 + 2 * nb: 0} if dq is not None and not last else {},
                compiler_params=pltpu.CompilerParams(vmem_limit_bytes=28 * 2 ** 20),
                cost_estimate=cost, name='attn_bwd')(*ins)

        kx, vx, ky, vy, q2, do2, lse2, delta, start, first = pl.pallas_call(
            functools.partial(prep_kernel, **dims),
            out_shape=tuple([sds((blk, d), bf16)] * 4 + [sds((2, n_sub * half, d), bf16)] * 2 + [sds((2, n_sub, half), f32)] * 2
                            + [sds((2, n_sub, half), i32), sds((8, n_sub), i32)]),
            in_specs=[hbm] * 7, out_specs=(vm,) * 10,
            scratch_shapes=[VMEM((2, n_sub * half, d), bf16), VMEM((2, n_sub, heads, loc), f32), VMEM((pad, 128), i32),
                            pltpu.SemaphoreType.DMA((8,)), pltpu.SemaphoreType.DMA((8,)), pltpu.SemaphoreType.DMA((5,))],
            compiler_params=pltpu.CompilerParams(collective_id=0, has_side_effects=True, vmem_limit_bytes=24 * 2 ** 20),
            name='prep',
        )(*[pltpu.with_memory_space_constraint(x, pltpu.HBM) for x in (
            k_own, v_own, query.reshape(-1, d), out_grad.reshape(-1, d), out_act.reshape(-1, d),
            row_lse.transpose(0, 2, 1), doc_ids.reshape(n_keys // 128, 128))])
        kd = swap(kx, 4)
        vd = swap(vy, 2)
        both = (('k', 0, None), ('v', 0, None))
        sides = ((2,), (4,))
        cut = blk // KT // 2 * KT
        four = (('k', 0, None), ('v', 1, None), ('k', 1, None), ('v', 0, None))
        dq, dk_xa, dv_ya, dk_ya, dv_xa = attend([kx, ky], [vx, vy], None, sides, four, 0, cut)
        got_ka = swap(dk_xa, 2)
        got_va = swap(dv_ya, 4)
        dq, dk_d, dv_d = attend([kd], [vd], dq, ((2, 4),), both)
        got_ky = swap(dk_d, 2)
        got_vx = swap(dv_d, 4)
        four = (('k', 0, None), ('v', 1, None), ('k', 1, 0), ('v', 0, 1))
        dq, dk_xb, dv_yb, dk_y, dv_x = attend([kx, ky], [vx, vy], dq, sides, four, cut, blk - cut, (dk_ya, dv_xa))
        got_kb = swap(dk_xb, 2)
        got_vb = swap(dv_yb, 4)
        last_k = swap(dk_y + got_ky, 4)
        last_v = swap(dv_x + got_vx, 2)
        dq_own, dq_other, dk_o, dv_o = attend([k_own], [v_own], dq, ((),), both, last=True)
        got_dq = swap(dq_other, 1)
        d_query = pl.pallas_call(
            functools.partial(finish_kernel, scale=scale), out_shape=sds((n_sub * half, d), bf16), in_specs=[vm, vm], out_specs=vm,
            compiler_params=pltpu.CompilerParams(vmem_limit_bytes=28 * 2 ** 20),
            cost_estimate=cost, name='finish_dq')(dq_own, got_dq)
        d_key, d_value = pl.pallas_call(
            functools.partial(sum_kernel, scale=scale, cut=cut), out_shape=(kv_out, kv_out), in_specs=[vm] * 8,
            out_specs=(pl.BlockSpec(memory_space=pltpu.HBM),) * 2,
            scratch_shapes=[VMEM((2, blk, d), f32), pltpu.SemaphoreType.DMA((2,))],
            compiler_params=pltpu.CompilerParams(vmem_limit_bytes=28 * 2 ** 20),
            cost_estimate=cost, name='sum_kv')(dk_o, got_ka, got_kb, last_k, dv_o, got_va, got_vb, last_v)
        return d_query.reshape(query.shape), d_key.reshape(key_act.shape), d_value.reshape(value_act.shape)

    return jax.shard_map(local_backward, mesh=mesh, in_specs=(q_spec, q_spec, q_spec, lse_spec, kv_spec, kv_spec, P()), out_specs=(q_spec, kv_spec, kv_spec), check_vma=False)
```

```python
import functools

import jax
import jax.numpy as jnp
from jax import lax
from jax.experimental import pallas as pl
from jax.experimental.pallas import tpu as pltpu
from jax.sharding import PartitionSpec as P


LOG2E = 1.4426950408889634
NT = (((1,), (1,)), ((), ()))
MESH = pl.DeviceIdType.MESH
VMEM, SMEM = pltpu.VMEM, pltpu.SMEM
HIGHEST = lax.Precision.HIGHEST
KT = 256
SMALL = 128
MAIN, MAIN_SMALL, TAIL = 6, 4, 2


def flip(me, bit):
    return me + bit - 2 * bit * lax.rem(me // bit, 2)


def prep_kernel(k_ref, v_ref, q_ref, do_ref, o_ref, lse_ref, ids_ref,
                kx_ref, vx_ref, ky_ref, vy_ref, q2_ref, do2_ref, lse2_ref, delta_ref, start_ref, first_ref,
                o2_ref, lraw_ref, mark_ref, send_sem, recv_sem, load_sem, *, pre, sub_len, loc, heads):
    me = lax.axis_index('cp')
    core = lax.rem(me, 2)
    nx, ny, partner = flip(me, 2), flip(me, 4), flip(me, 1)
    barrier = pltpu.get_barrier_semaphore()
    for other in (nx, ny, partner):
        pl.semaphore_signal(barrier, inc=1, device_id={'cp': other}, device_id_type=MESH)
    pl.semaphore_wait(barrier, 3)
    pairs = [(do_ref, do2_ref), (o_ref, o2_ref), (lse_ref, lraw_ref), (q_ref, q2_ref)]
    moves = [(s, r.at[core], partner) for s, r in pairs]
    moves += [(k_ref, kx_ref, nx), (v_ref, vy_ref, ny), (v_ref, vx_ref, nx), (k_ref, ky_ref, ny)]
    sends = [pltpu.make_async_remote_copy(src_ref=s, dst_ref=r, send_sem=send_sem.at[i], recv_sem=recv_sem.at[i],
                                          device_id={'cp': to}, device_id_type=MESH) for i, (s, r, to) in enumerate(moves)]
    loads = [pltpu.make_async_copy(s, r.at[core], load_sem.at[i]) for i, (s, r) in enumerate(pairs)]
    for copy in sends[4:] + sends[:4] + loads:
        copy.start()

    n_rows = ids_ref.shape[0]
    n_sub = lraw_ref.shape[1]
    pad = mark_ref.shape[0]
    load_ids = pltpu.make_async_copy(ids_ref, mark_ref.at[pl.ds(0, n_rows)], load_sem.at[4])
    load_ids.start()
    mark_ref[pl.ds(n_rows, pad - n_rows), :] = jnp.zeros((pad - n_rows, 128), jnp.int32)
    load_ids.wait()
    ids = mark_ref[...]
    lane = lax.broadcasted_iota(jnp.int32, (pad, 128), 1)
    row = lax.broadcasted_iota(jnp.int32, (pad, 128), 0)
    prev = pltpu.roll(ids, 1, axis=1)
    prev = jnp.where(lane == 0, pltpu.roll(prev, 1, axis=0), prev)
    acc = jnp.where(ids != prev, row * 128 + lane, 0)
    for sh in (1, 2, 4, 8, 16, 32, 64):
        acc = jnp.maximum(acc, jnp.where(lane >= sh, pltpu.roll(acc, sh, axis=1), 0))
    carry = jnp.max(acc, axis=1, keepdims=True) + jnp.zeros((pad, 128), jnp.int32)
    carry = jnp.where(row >= 1, pltpu.roll(carry, 1, axis=0), 0)
    sh = 1
    while sh < pad:
        carry = jnp.maximum(carry, jnp.where(row >= sh, pltpu.roll(carry, sh, axis=0), 0))
        sh *= 2
    starts = jnp.maximum(acc, carry).astype(jnp.float32)

    def hdot(a, b, dims=None):
        dims = (((1,), (0,)), ((), ())) if dims is None else dims
        return lax.dot_general(a, b, dims, precision=HIGHEST, preferred_element_type=jnp.float32)

    per = sub_len // 128
    off = (me // 2) * 2 * loc
    r_sub = lax.broadcasted_iota(jnp.int32, (n_sub, pad), 0)
    r_row = lax.broadcasted_iota(jnp.int32, (n_sub, pad), 1)
    pick = jnp.where(r_row == pre // 128 + per * r_sub + off // 128, 1.0, 0.0)
    sub_starts = hdot(pick, starts)
    src = lax.broadcasted_iota(jnp.int32, (128, 128), 0)
    dst = lax.broadcasted_iota(jnp.int32, (128, 128), 1)
    for e in range(2):
        spread = jnp.where(src == lax.rem(off, 128) + e * loc + dst // heads, 1.0, 0.0)
        rows_start = hdot(sub_starts, spread)
        start_ref[e] = rows_start.astype(jnp.int32)
        if e == 0:
            head = jnp.where(lax.broadcasted_iota(jnp.int32, (8, 128), 1) == 0, 1.0, 0.0)
            firsts = hdot(head, jnp.concatenate([rows_start, jnp.zeros((128 - n_sub, 128), jnp.float32)]), NT).astype(jnp.int32)
            tile = lax.broadcasted_iota(jnp.int32, (8, 128), 1)
            low = lax.broadcasted_iota(jnp.int32, (8, 128), 0) * k_ref.shape[0]
            hi = jnp.minimum(pre + off + tile * sub_len + 2 * loc - 1, low + k_ref.shape[0] - 1)
            span = (hi - jnp.maximum(firsts, low)).astype(jnp.float32)
            work = jnp.where((tile < n_sub) & (span >= 0), span * (1.0 / KT) + 0.5, 0.0)
            work = jnp.sum(work, axis=1, keepdims=True).astype(jnp.int32)
            first_ref[...] = jnp.where(tile < n_sub, firsts, work)

    def delta_of(e, o_part):
        def body(t, c):
            r0 = pl.multiple_of(t * 128, 128)
            prod = do2_ref[e, pl.ds(r0, 128), :].astype(jnp.float32) * o_part[pl.ds(r0, 128), :].astype(jnp.float32)
            delta_ref[e, pl.ds(t, 1), :] = jnp.sum(prod.T, axis=0, keepdims=True)
            return c

        lax.fori_loop(0, n_sub, body, 0)

    for load in loads:
        load.wait()
    delta_of(core, o2_ref.at[core])
    for copy in sends[:3]:
        copy.wait_recv()
    delta_of(1 - core, o2_ref.at[1 - core])
    tok = lax.broadcasted_iota(jnp.int32, (loc, 128), 0)
    tok_lane = lax.broadcasted_iota(jnp.int32, (loc, 128), 1)
    tok_spread = jnp.where(tok == tok_lane // heads, 1.0, 0.0)
    head_of = lax.broadcasted_iota(jnp.int32, (n_sub * heads, 128), 0)
    head_lane = lax.broadcasted_iota(jnp.int32, (n_sub * heads, 128), 1)
    own_head = lax.rem(head_of, heads) == lax.rem(head_lane, heads)
    g_sub = lax.broadcasted_iota(jnp.int32, (n_sub, n_sub * heads), 0)
    g_row = lax.broadcasted_iota(jnp.int32, (n_sub, n_sub * heads), 1)
    group = jnp.where(g_row // heads == g_sub, 1.0, 0.0)
    for e in range(2):
        wide = hdot(lraw_ref[e].reshape(n_sub * heads, loc), tok_spread)
        lse2_ref[e] = hdot(group, jnp.where(own_head, wide, 0.0)) * LOG2E
    for copy in sends[3:]:
        copy.wait_recv()
    for copy in sends:
        copy.wait_send()


def finish_kernel(own_ref, got_ref, out_ref, *, scale):
    half = own_ref.shape[2]

    step = 4

    def put(i, c):
        for u in range(step):
            t = i * step + u
            total = (own_ref[t] + got_ref[t]) * scale
            out_ref[pl.ds(pl.multiple_of(t * half, half), half), :] = total.T.astype(jnp.bfloat16)
        return c

    lax.fori_loop(0, own_ref.shape[0] // step, put, 0)


def sum_kernel(dk_ref, ka_ref, kb_ref, lk_ref, dv_ref, va_ref, vb_ref, lv_ref, dk_out, dv_out, sum_ref, sem, *, scale, cut):
    n = dk_ref.shape[0]
    copies = []
    for i, (own, a, b, end, out, mul) in enumerate([(dk_ref, ka_ref, kb_ref, lk_ref, dk_out, scale), (dv_ref, va_ref, vb_ref, lv_ref, dv_out, 1.0)]):
        sum_ref[i, 0:cut, :] = (own[0:cut, :] + a[...] + end[0:cut, :]) * mul
        sum_ref[i, cut:n, :] = (own[cut:n, :] + b[...] + end[cut:n, :]) * mul
        copies.append(pltpu.make_async_copy(sum_ref.at[i], out, sem.at[i]))
        copies[-1].start()
    for copy in copies:
        copy.wait()


def attn_kernel(*refs, blocks, row0, n_keys, outs, n_prev, has_dq, last, early, scale, blk, pre, sub_len, loc, heads):
    first_ref, q_ref, do_ref, lse_ref, delta_ref, start_ref = refs[:6]
    nb = len(blocks)
    k_in, v_in, refs = refs[6:6 + nb], refs[6 + nb:6 + 2 * nb], refs[6 + 2 * nb:]
    if has_dq:
        dq_in, refs = refs[0], refs[1:]
    prev, refs = refs[:n_prev], refs[n_prev:]
    if early:
        k_own, v_own = prev
    n_dq = 2 if last else 1
    dq_out, grad_out, refs = refs[:n_dq], refs[n_dq:n_dq + len(outs)], refs[n_dq + len(outs):]
    it_t, it_k, it_lo, it_base, p_ref, ds_ref, kpos_ref, refs = *refs[:7], refs[7:]
    if last:
        dq_ref, refs = refs[0], refs[1:]
    else:
        dq_ref = dq_out[0]
    if nb == 1:
        k_ref, v_ref, dk_ref, dv_ref = k_in[0], v_in[0], grad_out[0], grad_out[1]
        if early:
            own = k_own, v_own, grad_out[2], grad_out[3]
    else:
        k_ref, v_ref, dk_ref, dv_ref = refs
    me = lax.axis_index('cp')
    n_sub, half = lse_ref.shape[1], lse_ref.shape[2]
    rows = 2 * half
    pos0 = pre + (me // 2) * 2 * loc
    if nb > 1:
        for b in range(nb):
            k_ref[b * n_keys:(b + 1) * n_keys, :] = k_in[b][row0:row0 + n_keys, :]
            v_ref[b * n_keys:(b + 1) * n_keys, :] = v_in[b][row0:row0 + n_keys, :]
    if not last:
        dk_ref[...] = jnp.zeros_like(dk_ref)
        dv_ref[...] = jnp.zeros_like(dv_ref)
    if early:
        own[2][...] = jnp.zeros_like(own[2])
        own[3][...] = jnp.zeros_like(own[3])
    if last:
        dq_ref[...] = dq_in[...]
    elif not has_dq:
        dq_ref[...] = jnp.zeros_like(dq_ref)

    cap = it_t.shape[0] // 2

    def put_item(m, t, b, row, lo, blo, kt):
        it_t[m] = t
        it_k[m] = b * n_keys + jnp.minimum(row, n_keys - kt)
        it_lo[m] = lo
        it_base[m] = blo - b * n_keys

    def owner_of(bits):
        owner = me
        for bit in bits:
            owner = flip(owner, bit)
        return owner

    def build(blocks):
        n_items, n_small = 0, 0
        for b, bits in enumerate(blocks):
            blo = owner_of(bits) * blk + row0

            def more(c, blo=blo):
                return (c[0] < n_sub) & (first_ref[0, jnp.minimum(c[0], n_sub - 1)] < blo + n_keys)

            def add_tile(c, b=b, blo=blo):
                t, n, ns = c
                lo = jnp.maximum(first_ref[0, t], blo)
                hi = jnp.minimum(pos0 + t * sub_len + 2 * loc - 1, blo + n_keys - 1)
                off = (lo - blo) // 16 * 16
                length = hi - blo - off + 1
                full = length // KT
                rest = length - full * KT
                cnt = full + jnp.where(rest > SMALL, 1, 0)

                def add_item(i, m):
                    put_item(m, t, b, off + i * KT, blo + off + i * KT, blo, KT)
                    return m + 1

                put_item(cap + ns, t, b, off + full * KT, blo + off + full * KT, blo, SMALL)
                ns = ns + jnp.where((rest > 0) & (rest <= SMALL), 1, 0)
                return t + 1, lax.fori_loop(0, cnt, add_item, n), ns

            t_first = jnp.maximum(blo - pos0 - 2 * loc + sub_len, 0) // sub_len
            _, n_items, n_small = lax.while_loop(more, add_tile, (t_first, n_items, n_small))
        for n in (n_items, cap + n_small):
            put_item(n, 0, 0, 0, 1 << 30, 0, KT)
        return n_items, n_small

    def two(ref, t):
        return jnp.concatenate([ref[0, pl.ds(t, 1), :], ref[1, pl.ds(t, 1), :]], axis=1)

    lane = lax.broadcasted_iota(jnp.int32, (1, rows), 1)
    zero = jnp.zeros((16, rows), jnp.bfloat16)
    kpos_ref[...] = lax.broadcasted_iota(jnp.int32, (KT, rows), 0).astype(jnp.float32).astype(jnp.bfloat16)

    def item(m):
        t = it_t[m]
        k0 = pl.multiple_of(it_k[m], 16)
        r0 = pl.multiple_of(t * half, half)
        q = jnp.concatenate([q_ref[0, pl.ds(r0, half), :], q_ref[1, pl.ds(r0, half), :]], axis=0)
        do = jnp.concatenate([do_ref[0, pl.ds(r0, half), :], do_ref[1, pl.ds(r0, half), :]], axis=0)
        return t, k0, q, do

    def scores(first, n, kt, refs):
        k_ref, v_ref = refs[:2]
        out = []
        for u in range(n):
            m = first + u
            t, k0, q, do = item(m)
            s = lax.dot_general(k_ref[pl.ds(k0, kt), :], q, NT, preferred_element_type=jnp.float32)
            dp = lax.dot_general(v_ref[pl.ds(k0, kt), :], do, NT, preferred_element_type=jnp.float32)
            lo = jnp.maximum(two(start_ref, t), it_lo[m]) - (k0 + it_base[m])
            qpos = lane // heads + (pos0 + t * sub_len - k0 - it_base[m])
            lo = packed(jnp.clip(lo, 0, KT))
            qpos = packed(jnp.clip(qpos, -1, KT))
            out.append((s, dp, lo, qpos, two(lse_ref, t), two(delta_ref, t)))
        return out

    def packed(x):
        return jnp.broadcast_to(x.astype(jnp.float32), (16, rows)).astype(jnp.bfloat16)

    def probs(parts, kt):
        for u in range(len(parts)):
            s, dp, lo, qpos, lse, delta = parts[u]
            for g in range(kt // 16):
                r = slice(16 * g, 16 * g + 16)
                kpos = kpos_ref[r, :]
                allowed = (kpos >= lo) & (kpos <= qpos)
                p = jnp.exp2(s[r, :] * (scale * LOG2E) - lse)
                ds = p * (dp[r, :] - delta)
                p_ref[u, r, :] = jnp.where(allowed, p.astype(jnp.bfloat16), zero)
                ds_ref[u, r, :] = jnp.where(allowed, ds.astype(jnp.bfloat16), zero)

    def grads(first, n, kt, refs):
        k_ref, _, dk_ref, dv_ref = refs
        for u in range(n):
            t, k0, q, do = item(first + u)
            p, ds = p_ref[u, :kt, :], ds_ref[u, :kt, :]
            dv_ref[pl.ds(k0, kt), :] += jnp.dot(p, do, preferred_element_type=jnp.float32)
            dk_ref[pl.ds(k0, kt), :] += jnp.dot(ds, q, preferred_element_type=jnp.float32)
            dq_ref[t] += jnp.dot(k_ref[pl.ds(k0, kt), :].T, ds, preferred_element_type=jnp.float32)

    def loop(first, n, count, kt, refs):
        def body(w, c):
            m = first + w * n
            probs(scores(m, n, kt, refs), kt)
            grads(m, n, kt, refs)
            return c

        lax.fori_loop(0, count, body, 0)

    def spare():
        core = lax.rem(me, 2)
        most = 0
        for j in range(4):
            most = jnp.maximum(most, first_ref[2 * j + core, n_sub])
        groups = (most - first_ref[owner_of((2, 4)), n_sub]) // MAIN
        return jnp.maximum(groups - 1, 0)

    refs = k_ref, v_ref, dk_ref, dv_ref
    n_items, n_small = build(blocks)
    start_main = jnp.minimum(spare(), n_items // MAIN) if last else 0
    n_main = n_items // MAIN
    loop(start_main * MAIN, MAIN, n_main - start_main, KT, refs)
    loop(n_main * MAIN, TAIL, (n_items - n_main * MAIN + TAIL - 1) // TAIL, KT, refs)
    n_main = n_small // MAIN_SMALL
    loop(cap, MAIN_SMALL, n_main, SMALL, refs)
    loop(cap + n_main * MAIN_SMALL, TAIL, (n_small - n_main * MAIN_SMALL + TAIL - 1) // TAIL, SMALL, refs)
    if early:
        groups = spare()

        @pl.when(groups > 0)
        def _():
            n_own, _ = build(((),))
            loop(0, MAIN, jnp.minimum(groups, n_own // MAIN), KT, own)

    if nb > 1:
        for ref, (kind, b, i) in zip(grad_out, outs):
            acc = dk_ref if kind == 'k' else dv_ref
            if i is None:
                ref[...] = acc[b * n_keys:(b + 1) * n_keys, :]
            else:
                ref[0:row0, :] = prev[i][...]
                ref[row0:row0 + n_keys, :] = acc[b * n_keys:(b + 1) * n_keys, :]
    if last:
        core = lax.rem(me, 2)
        mine = pl.multiple_of(core * half, half)
        theirs = pl.multiple_of((1 - core) * half, half)

        def put(t, c):
            dq_out[0][t] = dq_ref[t, :, pl.ds(mine, half)]
            dq_out[1][t] = dq_ref[t, :, pl.ds(theirs, half)]
            return c

        lax.fori_loop(0, n_sub, put, 0)


def solution(mesh):
    cp = mesh.shape['cp']
    q_spec = P(None, 'cp', 'tp', None)
    lse_spec = P(None, 'cp', 'tp')
    kv_spec = P('cp', 'tp', None)

    def swap(x, bits):
        return lax.ppermute(x, 'cp', [(i, i ^ bits) for i in range(cp)])

    def local_backward(query, out_act, out_grad, row_lse, key_act, value_act, doc_ids):
        n_sub, loc, heads, d = query.shape
        blk = key_act.shape[0]
        n_keys = blk * cp
        half = loc * heads
        sub_len = loc * cp
        pre = n_keys - n_sub * sub_len
        scale = d ** -0.5
        f32, bf16, i32 = jnp.float32, jnp.bfloat16, jnp.int32
        dims = dict(pre=pre, sub_len=sub_len, loc=loc, heads=heads)
        vm = pl.BlockSpec(memory_space=VMEM)
        sm = pl.BlockSpec(memory_space=SMEM)
        hbm = pl.BlockSpec(memory_space=pltpu.HBM)
        sds = jax.ShapeDtypeStruct
        k_own, v_own = key_act.reshape(blk, d), value_act.reshape(blk, d)
        pad = (n_keys // 128 + 7) // 8 * 8
        acc = sds((n_sub, d, 2 * half), f32)
        kv_out = sds((blk, d), f32)
        dq_half = sds((n_sub, d, half), f32)
        cost = pl.CostEstimate(flops=2 * 10 ** 9, bytes_accessed=10 ** 7, transcendentals=10 ** 6)

        def attend(keys, values, dq, blocks, outs, row0=0, n_rows=blk, prev=(), last=False, early=False):
            nb = len(blocks)
            ins = [first, q2, do2, lse2, delta, start, *keys, *values] + ([dq] if dq is not None else []) + list(prev)
            cap = nb * n_sub * (-(-n_rows // KT) + 1) + TAIL
            kv = (nb * n_rows, d)
            dq_shapes = (dq_half, dq_half) if last else (acc,)
            scratch = [SMEM((2 * cap,), i32)] * 4 + [VMEM((MAIN, KT, 2 * half), bf16)] * 2 + [VMEM((KT, 2 * half), bf16)]
            scratch += [VMEM((n_sub, d, 2 * half), f32)] if last else []
            scratch += [VMEM(kv, bf16)] * 2 + [VMEM(kv, f32)] * 2 if nb > 1 else []
            alias = {7 + 2 * nb: 2, 8 + 2 * nb: 3} if last else {6 + 2 * nb: 0} if dq is not None else {}
            return pl.pallas_call(
                functools.partial(attn_kernel, blocks=blocks, row0=row0, n_keys=n_rows, outs=outs, n_prev=len(prev),
                                  has_dq=dq is not None, last=last, early=early,
                                  scale=scale, blk=blk, **dims),
                out_shape=dq_shapes + tuple(sds((n_rows if i is None else row0 + n_rows, d), f32) for _, _, i in outs),
                in_specs=[sm] + [vm] * (len(ins) - 1), out_specs=(vm,) * (len(dq_shapes) + len(outs)),
                scratch_shapes=scratch, input_output_aliases=alias,
                compiler_params=pltpu.CompilerParams(vmem_limit_bytes=28 * 2 ** 20),
                cost_estimate=cost, name='attn_bwd')(*ins)

        kx, vx, ky, vy, q2, do2, lse2, delta, start, first = pl.pallas_call(
            functools.partial(prep_kernel, **dims),
            out_shape=tuple([sds((blk, d), bf16)] * 4 + [sds((2, n_sub * half, d), bf16)] * 2 + [sds((2, n_sub, half), f32)] * 2
                            + [sds((2, n_sub, half), i32), sds((8, 128), i32)]),
            in_specs=[hbm] * 7, out_specs=(vm,) * 10,
            scratch_shapes=[VMEM((2, n_sub * half, d), bf16), VMEM((2, n_sub, heads, loc), f32), VMEM((pad, 128), i32),
                            pltpu.SemaphoreType.DMA((8,)), pltpu.SemaphoreType.DMA((8,)), pltpu.SemaphoreType.DMA((5,))],
            compiler_params=pltpu.CompilerParams(collective_id=0, has_side_effects=True, vmem_limit_bytes=24 * 2 ** 20),
            name='prep',
        )(*[pltpu.with_memory_space_constraint(x, pltpu.HBM) for x in (
            k_own, v_own, query.reshape(-1, d), out_grad.reshape(-1, d), out_act.reshape(-1, d),
            row_lse.transpose(0, 2, 1), doc_ids.reshape(n_keys // 128, 128))])
        kd = swap(kx, 4)
        vd = swap(vy, 2)
        both = (('k', 0, None), ('v', 0, None))
        sides = ((2,), (4,))
        cut = blk // KT // 2 * KT
        four = (('k', 0, None), ('v', 1, None), ('k', 1, None), ('v', 0, None))
        dq, dk_xa, dv_ya, dk_ya, dv_xa = attend([kx, ky], [vx, vy], None, sides, four, 0, cut)
        got_ka = swap(dk_xa, 2)
        got_va = swap(dv_ya, 4)
        dq, dk_d, dv_d, dk_o, dv_o = attend([kd], [vd], dq, ((2, 4),), both * 2, prev=(k_own, v_own), early=True)
        got_ky = swap(dk_d, 2)
        got_vx = swap(dv_d, 4)
        four = (('k', 0, None), ('v', 1, None), ('k', 1, 0), ('v', 0, 1))
        dq, dk_xb, dv_yb, dk_y, dv_x = attend([kx, ky], [vx, vy], dq, sides, four, cut, blk - cut, (dk_ya, dv_xa))
        got_kb = swap(dk_xb, 2)
        got_vb = swap(dv_yb, 4)
        last_k = swap(dk_y + got_ky, 4)
        last_v = swap(dv_x + got_vx, 2)
        dq_own, dq_other, dk_o, dv_o = attend([k_own], [v_own], dq, ((),), both, prev=(dk_o, dv_o), last=True)
        got_dq = swap(dq_other, 1)
        d_query = pl.pallas_call(
            functools.partial(finish_kernel, scale=scale), out_shape=sds((n_sub * half, d), bf16), in_specs=[vm, vm], out_specs=vm,
            compiler_params=pltpu.CompilerParams(vmem_limit_bytes=28 * 2 ** 20),
            cost_estimate=cost, name='finish_dq')(dq_own, got_dq)
        d_key, d_value = pl.pallas_call(
            functools.partial(sum_kernel, scale=scale, cut=cut), out_shape=(kv_out, kv_out), in_specs=[vm] * 8,
            out_specs=(pl.BlockSpec(memory_space=pltpu.HBM),) * 2,
            scratch_shapes=[VMEM((2, blk, d), f32), pltpu.SemaphoreType.DMA((2,))],
            compiler_params=pltpu.CompilerParams(vmem_limit_bytes=28 * 2 ** 20),
            cost_estimate=cost, name='sum_kv')(dk_o, got_ka, got_kb, last_k, dv_o, got_va, got_vb, last_v)
        return d_query.reshape(query.shape), d_key.reshape(key_act.shape), d_value.reshape(value_act.shape)

    return jax.shard_map(local_backward, mesh=mesh, in_specs=(q_spec, q_spec, q_spec, lse_spec, kv_spec, kv_spec, P()), out_specs=(q_spec, kv_spec, kv_spec), check_vma=False)
```
